256 devices in a mesh: seq: 32 (over x_lo, z, core), head: 8 (over x_hi, y).
Axes of the slice: x: 4 (x_hi: 2, x_lo: 2; x = x_hi * 2 + x_lo), y: 4, z: 8, core: 2. Of those that a mesh axis runs over, the one named last changes fastest.
Arguments:
- hidden: bfloat16 [9216, 8192], P('seq'), may hold values from -6 to 6
- norm_gain: bfloat16 [8192], replicated, may hold values from 0.099609375 to 1.8984375
- w_query: bfloat16 [8192, 4096], P('seq', 'head'), may hold values from -0.125 to 0.125
- w_key: bfloat16 [8192, 1024], P('seq', 'head'), may hold values from -0.125 to 0.125
- w_value: bfloat16 [8192, 1024], P('seq', 'head'), may hold values from -0.0625 to 0.0625
- bias_query: bfloat16 [4096], P('head'), may hold values from -3 to 3
- bias_key: bfloat16 [1024], P('head'), may hold values from -200 to 200
- bias_value: bfloat16 [1024], P('head'), may hold values from -3 to 3
- w_out: bfloat16 [4096, 8192], P('head', 'seq'), may hold values from -0.09375 to 0.09375
Outputs:
- attn_out: bfloat16 [9216, 8192], P(('seq', 'head'))
The draws below stay inside these ranges and needn't reach their ends.
All inputs are finite; a program needn't handle non-finite values.
Results may differ from the reference program's by a relative error of at most 0.014.
The reference program's roundings to bfloat16 on the way count: a program that leaves them out, or rounds other values in their place, can miss the bound.
Values may be sent and summed in bfloat16 or wider, within the bound.
A program may use at most 192 MiB of HBM per device.

```python
import jax
import jax.numpy as jnp
from jax import lax

D = 8192
HEAD_DIM = 128
QPG = 4
KV_HEADS = 8
LENGTH = 9216


def draw_bias_key(key, part):
    count = KV_HEADS * HEAD_DIM
    base = jax.random.normal(key, (count,), jnp.float32)
    return jnp.clip(0.5 * base, -3.0, 3.0).astype(jnp.bfloat16)


def steps_of(own_key, extent, split, least, high):
    gain = 1.0
    for position, shards_of in split:
        heights = jax.random.uniform(jax.random.fold_in(jax.random.fold_in(own_key, 6), position), (shards_of,), jnp.float32, least / len(split), high / len(split))
        gain = gain * jnp.repeat(jnp.exp(heights), extent[position] // shards_of).reshape((-1,) + (1,) * (len(extent) - 1 - position))
    return gain


def noise(own_key, dims, deviation, limit, split=(), kind=jnp.bfloat16):
    values = deviation * jax.random.normal(own_key, dims, jnp.float32)
    if split:
        values = values * steps_of(own_key, dims, split, -0.22, 0.18)
    return jnp.clip(values, -limit, limit).astype(kind)


def setup_inputs(seed: int = 0) -> dict:
    key_of = jax.random.split(jax.random.key(seed), 10)
    hidden = noise(key_of[0], (LENGTH, D), 1.0, 6.0, ((0, 32),))
    norm_gain = jnp.clip(1.0 + 0.18 * jax.random.normal(key_of[1], (D,), jnp.float32), 0.099609375, 1.8984375).astype(jnp.bfloat16)
    w_query = noise(key_of[2], (D, KV_HEADS * QPG * HEAD_DIM), (D // 4) ** -0.5, 0.125, ((0, 32), (1, 8)))
    w_key = noise(key_of[3], (D, KV_HEADS * HEAD_DIM), (D // 4) ** -0.5, 0.125, ((0, 32), (1, 8)))
    w_value = noise(key_of[4], (D, KV_HEADS * HEAD_DIM), D ** -0.5, 0.0625, ((0, 32), (1, 8)))
    bias_query = noise(key_of[5], (KV_HEADS * QPG * HEAD_DIM,), 0.5, 3.0, ((0, 8),))
    bias_key = draw_bias_key(jax.random.fold_in(key_of[9], 71), 0)
    bias_value = noise(key_of[7], (KV_HEADS * HEAD_DIM,), 0.5, 3.0, ((0, 8),))
    w_out = noise(key_of[8], (KV_HEADS * QPG * HEAD_DIM, D), (KV_HEADS * QPG * HEAD_DIM) ** -0.5, 0.09375, ((0, 8), (1, 32)))
    return dict(hidden=hidden, norm_gain=norm_gain, w_query=w_query, w_key=w_key, w_value=w_value, bias_query=bias_query, bias_key=bias_key, bias_value=bias_value, w_out=w_out)


ROPE_BASE = 1000000.0
EPSILON = 1e-06

def rotary(values, positions):
    half = values.shape[-1] // 2
    freq = ROPE_BASE ** (-2.0 * jnp.arange(half, dtype=jnp.float32) / values.shape[-1])
    angles = positions.astype(jnp.float32)[:, None, None] * freq[None, None, :]
    cosine = jnp.cos(angles)
    sine = jnp.sin(angles)
    first = values[..., :half]
    second = values[..., half:]
    return jnp.concatenate([first * cosine - second * sine, second * cosine + first * sine], axis=-1)

def reference(hidden, norm_gain, w_query, w_key, w_value, bias_query, bias_key, bias_value, w_out):
    length = hidden.shape[0]
    widened = hidden.astype(jnp.float32)
    inverse = lax.rsqrt(lax.optimization_barrier(jnp.mean(widened * widened, axis=-1, keepdims=True)) + EPSILON)
    normed = (widened * inverse * norm_gain.astype(jnp.float32)).astype(jnp.bfloat16)
    positions = jnp.arange(length, dtype=jnp.int32)
    query = jnp.dot(normed, w_query, preferred_element_type=jnp.float32) + bias_query.astype(jnp.float32)
    keys = jnp.dot(normed, w_key, preferred_element_type=jnp.float32) + bias_key.astype(jnp.float32)
    values = jnp.dot(normed, w_value, preferred_element_type=jnp.float32) + bias_value.astype(jnp.float32)
    query = rotary(query.reshape(length, KV_HEADS * QPG, HEAD_DIM), positions).astype(jnp.bfloat16)
    keys = rotary(keys.reshape(length, KV_HEADS, HEAD_DIM), positions).astype(jnp.bfloat16)
    values = values.reshape(length, KV_HEADS, HEAD_DIM).astype(jnp.bfloat16)
    query_groups = query.reshape(length, KV_HEADS, QPG, HEAD_DIM).transpose(1, 2, 0, 3)
    key_groups = keys.transpose(1, 0, 2)
    value_groups = values.transpose(1, 0, 2)
    causal = positions[:, None] >= positions[None, :]
    out_groups = w_out.reshape(KV_HEADS, QPG * HEAD_DIM, w_out.shape[1])

    def attend(carry, group):
        group_query, group_key, group_value, group_out = group
        scores = jnp.einsum('hqd,kd->hqk', group_query.astype(jnp.float32), group_key.astype(jnp.float32)) * HEAD_DIM ** (-0.5)
        scores = jnp.where(causal[None], scores, -jnp.inf)
        highest = lax.optimization_barrier(jnp.max(scores, axis=-1, keepdims=True))
        probs = jnp.exp(scores - highest)
        total = lax.optimization_barrier(jnp.sum(probs, axis=-1, keepdims=True))
        rounded = lax.optimization_barrier(probs.astype(jnp.bfloat16))
        mixed = jnp.einsum('hqk,kd->hqd', rounded.astype(jnp.float32), group_value.astype(jnp.float32))
        attended = (mixed / total).astype(jnp.bfloat16)
        attended = attended.transpose(1, 0, 2).reshape(length, QPG * HEAD_DIM)
        term = jnp.dot(attended, group_out, preferred_element_type=jnp.float32)
        term = lax.optimization_barrier(term.astype(jnp.bfloat16))
        return (carry + term.astype(jnp.float32), None)
    start = jnp.zeros((length, w_out.shape[1]), jnp.float32)
    summed, unused = lax.scan(attend, start, (query_groups, key_groups, value_groups, out_groups))
    return summed.astype(jnp.bfloat16)
```

```python
import functools

import jax
import jax.numpy as jnp
from jax import lax
from jax.experimental import pallas as pl
from jax.experimental.pallas import tpu as pltpu
from jax.sharding import PartitionSpec as P

HEAD_DIM = 128
ROPE_BASE = 1000000.0
EPSILON = 1e-06
BF16 = jnp.bfloat16
F32 = jnp.float32
MESH = pl.DeviceIdType.MESH
ZS = 8
YS = 4
SEQ = 32
ROWS = 288
D = 8192
OWN = 36
GROUPS = 4
GCOLS = D // GROUPS
KBLOCK = 1152
PADROWS = 80
SCALE2 = HEAD_DIM**-0.5 * 1.4426950408889634


def wrap(value, size):
    return lax.rem(value + size, size)


class Gather:
    def __init__(self, kind, buf, rows, place, recv, sib_sem, send_sem):
        self.kind, self.buf, self.rows, self.half = kind, buf, rows, rows // 2
        self.x, self.z, self.c, self.head = place
        self.recv, self.sib_sem, self.send_sem = recv, sib_sem, send_sem
        self.zp = self.at(self.x, 1)
        self.zm = self.at(self.x, -1)
        self.xp = self.at(1 - self.x, 0)
        self.sib = (self.x * ZS + self.z) * 2 + 1 - self.c

    def at(self, x, dz):
        return (x * ZS + wrap(self.z + dz, ZS)) * 2 + self.c

    def copy(self, s, part, dev, sem):
        ref = self.buf.at[pl.ds(pl.multiple_of(s * self.rows + part * self.half, 16), self.half)]
        return pltpu.make_async_remote_copy(
            src_ref=ref,
            dst_ref=ref,
            send_sem=self.send_sem.at[self.kind],
            recv_sem=sem,
            device_id=(dev, self.head),
            device_id_type=MESH,
        )

    def sem(self, s, part):
        return self.recv.at[self.kind, lax.div(s, 2), part]

    def send(self, s, part, *devs):
        for dev in devs:
            self.copy(s, part, dev, self.sem(s, part)).start()
        self.copy(s, part, self.sib, self.sib_sem.at[self.kind]).start()

    def wait(self, s, part):
        self.copy(s, part, self.sib, self.sem(s, part)).wait_recv()

    def relay(self, s, part, *devs):
        self.wait(s, part)
        self.send(s, part, *devs)

    def own(self):
        s = self.at(self.x, 0)
        for part in (0, 1):
            self.send(s, part, self.zp, self.zm, self.xp)

    def cross(self):
        s = self.at(1 - self.x, 0)
        self.relay(s, 0, self.zp, self.zm)
        self.relay(s, 1)

    def step(self, k):
        lo, hi = self.at(self.x, -k), self.at(self.x, k)
        self.relay(lo, 0, self.zp)
        self.relay(hi, 0, self.zm)
        self.relay(lo, 1, self.zp, self.xp)
        self.relay(hi, 1, self.zm, self.xp)
        self.relay(self.at(1 - self.x, -k), 0, self.zp)
        self.relay(self.at(1 - self.x, k), 0, self.zm)

    def crossed(self, k):
        self.relay(self.at(1 - self.x, -k), 1)
        self.relay(self.at(1 - self.x, k), 1)

    def step3(self):
        lo, hi = self.at(self.x, -3), self.at(self.x, 3)
        self.relay(lo, 0, self.zp)
        self.relay(hi, 1, self.zm, self.xp)
        self.relay(lo, 1, self.xp)
        self.relay(hi, 0)
        self.relay(self.at(1 - self.x, -3), 0)
        self.relay(self.at(1 - self.x, 3), 0)

    def step4(self):
        far = self.at(self.x, 4)
        self.relay(far, 0, self.xp)
        self.relay(far, 1, self.xp)

    def last(self):
        far = self.at(1 - self.x, 4)
        self.relay(far, 0)
        self.relay(far, 1)

    def finish(self):
        part = self.buf.at[pl.ds(0, 16 * self.rows)]
        pltpu.make_async_copy(part, part, self.sib_sem.at[self.kind]).wait()

    def drain(self):
        part = self.buf.at[pl.ds(0, 31 * self.rows)]
        pltpu.make_async_copy(part, part, self.send_sem.at[self.kind]).wait()


def rotated(values, cs, sn):
    return values * cs + pltpu.roll(values, HEAD_DIM // 2, 1) * sn


def kernel(
    hidden, gain, wq_in, wk_in, wv_in, bq, bk, bv, wo_in, cs, sn, out,
    hid, wkv, wq, kv, wo, qacc, qs, tmp, att32, att, terms, r1, r2, xs, xr, tot, keep,
    local, recv, sib_sem, send_sem, rsem, r_send,
):
    s = lax.axis_index("seq")
    head = lax.axis_index("head")
    c = lax.rem(s, 2)
    chip = lax.div(s, 2)
    z = lax.rem(chip, ZS)
    x = lax.div(chip, ZS)
    y = lax.rem(head, YS)
    xh = lax.div(head, YS)
    place = (x, z, c, head)
    gather = functools.partial(Gather, place=place, recv=recv, sib_sem=sib_sem, send_sem=send_sem)
    g_kv_w = gather(0, wkv, 256)
    g_q_w = gather(1, wq, 256)
    g_kv = gather(2, kv, ROWS)
    g_o_w = gather(3, wo, 512)
    yp = xh * YS + wrap(y + 1, YS)
    ym = xh * YS + wrap(y - 1, YS)
    xhp = (1 - xh) * YS + y

    mine = pl.ds(pl.multiple_of(s * 256, 256), 256)
    mine_o = pl.ds(pl.multiple_of(s * 512, 512), 512)
    copies = [
        pltpu.make_async_copy(wk_in, wkv.at[mine, pl.ds(0, 128)], local.at[0]),
        pltpu.make_async_copy(wv_in, wkv.at[mine, pl.ds(128, 128)], local.at[1]),
        pltpu.make_async_copy(wq_in, wq.at[mine], local.at[2]),
        pltpu.make_async_copy(hidden, hid, local.at[3]),
        pltpu.make_async_copy(wo_in, wo.at[mine_o], local.at[4]),
    ]
    for copy in copies:
        copy.start()
    barrier = pltpu.get_barrier_semaphore()
    for dev in (g_q_w.zp, g_q_w.zm, g_q_w.xp, g_q_w.sib):
        pl.semaphore_signal(barrier, inc=1, device_id=(dev, head), device_id_type=MESH)
    for dev in (yp, ym, xhp):
        pl.semaphore_signal(barrier, inc=1, device_id=(s, dev), device_id_type=MESH)
    copies[0].wait()
    copies[1].wait()
    copies[2].wait()
    pl.semaphore_wait(barrier, 7)
    g_kv_w.own()
    g_q_w.own()

    copies[3].wait()

    @pl.loop(0, ROWS // 16)
    def _(i):
        rows = pl.ds(pl.multiple_of(i * 16, 16), 16)
        squares = jnp.zeros((16, 1024), F32)
        for j in range(8):
            part = hid[rows, pl.ds(j * 1024, 1024)].astype(F32)
            squares = squares + part * part
        inverse = lax.rsqrt(jnp.sum(squares, axis=-1, keepdims=True) * (1.0 / D) + EPSILON)
        for j in range(8):
            cols = pl.ds(j * 1024, 1024)
            part = hid[rows, cols].astype(F32)
            hid[rows, cols] = (part * inverse * gain[:, cols].astype(F32)).astype(BF16)

    def steps12(g):
        @pl.loop(1, 3)
        def _(k):
            g.step(k)

            @pl.when(k == 2)
            def _():
                g.crossed(1)

    def tail(g):
        g.step3()
        g.crossed(2)
        g.step4()
        g.crossed(3)
        g.last()

    g_kv_w.cross()
    steps12(g_kv_w)
    tail(g_kv_w)
    g_q_w.cross()
    g_kv_w.finish()

    def project(weights, cols):
        acc = qacc.at[:, pl.ds(0, cols)]
        acc[...] = jnp.zeros((ROWS, cols), F32)

        @pl.loop(0, 4)
        def _(i):
            depth = pl.ds(pl.multiple_of(i * 2048, 2048), 2048)
            acc[...] += jnp.dot(hid[:, depth], weights[depth, :], preferred_element_type=F32)

    project(wkv, 256)
    own_kv = pl.ds(pl.multiple_of(s * ROWS, 16), ROWS)
    kv[own_kv, 0:128] = rotated(qacc[:, 0:128] + bk[...].astype(F32), cs[...], sn[...]).astype(BF16)
    kv[own_kv, 128:256] = (qacc[:, 128:256] + bv[...].astype(F32)).astype(BF16)
    g_q_w.step(1)
    g_kv.own()
    g_q_w.step(2)
    g_q_w.crossed(1)
    g_kv.cross()
    g_q_w.step3()
    g_q_w.crossed(2)
    g_kv.step(1)
    g_q_w.step4()
    g_q_w.crossed(3)
    g_kv.step(2)
    g_kv.crossed(1)
    g_q_w.last()
    tail(g_kv)
    copies[4].wait()
    g_o_w.own()
    g_q_w.finish()
    project(wq, 512)
    for j in range(4):
        cols = pl.ds(j * HEAD_DIM, HEAD_DIM)
        value = qacc[:, cols] + bq[:, cols].astype(F32)
        qs[pl.ds(j * ROWS, ROWS), :] = rotated(value, cs[...], sn[...]).astype(BF16)
    g_kv.finish()
    g_o_w.cross()

    last_block = lax.div(s, 4)
    att32[...] = jnp.zeros(att32.shape, F32)

    @pl.loop(0, 4)
    def _(j):
        query = qs[pl.ds(pl.multiple_of(j * ROWS, 16), ROWS), :]

        def scores_of(block):
            keys = kv[pl.ds(pl.multiple_of(block * KBLOCK, KBLOCK), KBLOCK), 0:128]
            return lax.dot_general(query, keys, (((1,), (1,)), ((), ())), preferred_element_type=F32)

        def mixed(probs, block):
            values = kv[pl.ds(pl.multiple_of(block * KBLOCK, KBLOCK), KBLOCK), 128:256]
            return jnp.dot(probs.astype(BF16), values, preferred_element_type=F32)

        scores = scores_of(last_block)
        query_pos = s * ROWS + lax.broadcasted_iota(jnp.int32, (ROWS, KBLOCK), 0)
        key_pos = last_block * KBLOCK + lax.broadcasted_iota(jnp.int32, (ROWS, KBLOCK), 1)
        scores = jnp.where(query_pos >= key_pos, scores, -jnp.inf)
        highest = jnp.max(scores, axis=-1, keepdims=True)
        probs = jnp.exp2((scores - highest) * SCALE2)
        total = jnp.sum(probs, axis=-1, keepdims=True)
        summed = mixed(probs, last_block)

        def update(block, state):
            highest, total, summed = state
            scores = scores_of(block)
            new_high = jnp.maximum(highest, jnp.max(scores, axis=-1, keepdims=True))
            probs = jnp.exp2((scores - new_high) * SCALE2)
            fade = jnp.exp2((highest - new_high) * SCALE2)
            total = total * fade + jnp.sum(probs, axis=-1, keepdims=True)
            return new_high, total, summed * fade + mixed(probs, block)

        highest, total, summed = lax.fori_loop(0, last_block, update, (highest, total, summed))
        tmp[...] = summed / total
        cols = pl.ds(pl.multiple_of(j * HEAD_DIM, HEAD_DIM), HEAD_DIM)
        for h in range(8):
            spot = PADROWS * (h % YS) + OWN * (h // YS)
            att32[pl.ds(spot, OWN), cols] = tmp[pl.ds(h * OWN, OWN), :]

        @pl.when(j < 2)
        def _():
            g_o_w.step(j + 1)

        @pl.when(j == 2)
        def _():
            g_o_w.crossed(1)
            g_o_w.step3()

        @pl.when(j == 3)
        def _():
            g_o_w.crossed(2)
            g_o_w.step4()

    att[...] = att32[...].astype(BF16)
    g_o_w.crossed(3)
    g_o_w.last()
    g_o_w.finish()

    y2 = wrap(y + 2, YS)
    y_next = wrap(y + 1, YS)
    y_prev = wrap(y - 1, YS)
    half_cols = GCOLS // 2

    def move(src, dst, kind, g, dev):
        return pltpu.make_async_remote_copy(
            src_ref=src,
            dst_ref=dst,
            send_sem=r_send.at[kind, g],
            recv_sem=rsem.at[kind, g],
            device_id=(s, dev),
            device_id_type=MESH,
        )

    def first(g, kind):
        cols = pl.ds(g * GCOLS + kind * half_cols, half_cols)
        return move(terms.at[y2, :, cols], r1.at[kind, g], kind, g, ym if kind else yp)

    def second(g, kind):
        cols = pl.ds(g * GCOLS, GCOLS)
        row = y_prev if kind else y_next
        return move(terms.at[row, :, cols], r2.at[kind, g], 2 + kind, g, ym if kind else yp)

    def third(g):
        return move(xs.at[g], xr.at[g], 4, g, xhp)

    def compute(g):
        @pl.loop(0, GCOLS // 256)
        def _(i):
            slot = g * (GCOLS // 256) + i
            depth = pl.ds(pl.multiple_of(slot * 512, 512), 512)
            cols = pl.ds(pl.multiple_of(slot * 256, 256), 256)
            term = jnp.dot(att[...], wo[depth, :], preferred_element_type=F32).astype(BF16)
            for k in range(YS):
                terms[k, :, cols] = term[PADROWS * k : PADROWS * k + 2 * OWN]

        first(g, 0).start()
        first(g, 1).start()

    def pair(g):
        for kind in (0, 1):
            first(g, kind).wait_recv()
            row = y_prev if kind else y_next
            cols = pl.ds(g * GCOLS + kind * half_cols, half_cols)
            terms[row, :, cols] = (terms[row, :, cols].astype(F32) + r1[kind, g].astype(F32)).astype(BF16)
            second(g, kind).start()

    def across(g):
        second(g, 0).wait_recv()
        second(g, 1).wait_recv()
        cols = pl.ds(g * GCOLS, GCOLS)
        tot[...] = terms[y, :, cols].astype(F32) + r2[0, g].astype(F32) + r2[1, g].astype(F32)
        low, high = tot[0:OWN, :], tot[OWN : 2 * OWN, :]
        lower = xh == 0
        xs[g] = jnp.where(lower, high, low).astype(BF16)
        keep[g] = jnp.where(lower, low, high)
        third(g).start()

    def done(g):
        third(g).wait_recv()
        out[:, pl.ds(g * GCOLS, GCOLS)] = (keep[g] + xr[g].astype(F32)).astype(BF16)

    for t in range(GROUPS + 3):
        for lag, stage in enumerate((compute, pair, across, done)):
            if 0 <= t - lag < GROUPS:
                stage(t - lag)

    for g in range(GROUPS):
        for kind in (0, 1):
            first(g, kind).wait_send()
            second(g, kind).wait_send()
        third(g).wait_send()
    for g in (g_kv_w, g_q_w, g_kv, g_o_w):
        g.drain()


def local(hidden, norm_gain, w_query, w_key, w_value, bias_query, bias_key, bias_value, w_out):
    first_row = lax.axis_index("seq") * ROWS
    positions = first_row + jnp.arange(ROWS, dtype=jnp.int32)
    half_dim = HEAD_DIM // 2
    freq = ROPE_BASE ** (-2.0 * jnp.arange(half_dim, dtype=F32) / HEAD_DIM)
    angles = positions.astype(F32)[:, None] * freq[None, :]
    cosine, sine = jnp.cos(angles), jnp.sin(angles)
    cs = jnp.concatenate([cosine, cosine], axis=-1)
    sn = jnp.concatenate([-sine, sine], axis=-1)
    vmem = pl.BlockSpec(memory_space=pltpu.VMEM)
    hbm = pl.BlockSpec(memory_space=pl.ANY)
    dma = pltpu.SemaphoreType.DMA
    return pl.pallas_call(
        kernel,
        name="layer",
        out_shape=jax.ShapeDtypeStruct((OWN, D), BF16),
        in_specs=[hbm, vmem, hbm, hbm, hbm, vmem, vmem, vmem, hbm, vmem, vmem],
        out_specs=vmem,
        scratch_shapes=[
            pltpu.VMEM((ROWS, D), BF16),
            pltpu.VMEM((D, 256), BF16),
            pltpu.VMEM((D, 512), BF16),
            pltpu.VMEM((SEQ * ROWS, 256), BF16),
            pltpu.VMEM((SEQ * 512, 256), BF16),
            pltpu.VMEM((ROWS, 512), F32),
            pltpu.VMEM((4 * ROWS, HEAD_DIM), BF16),
            pltpu.VMEM((ROWS, HEAD_DIM), F32),
            pltpu.VMEM((YS * PADROWS, 512), F32),
            pltpu.VMEM((YS * PADROWS, 512), BF16),
            pltpu.VMEM((YS, 2 * OWN, D), BF16),
            pltpu.VMEM((2, GROUPS, 2 * OWN, GCOLS // 2), BF16),
            pltpu.VMEM((2, GROUPS, 2 * OWN, GCOLS), BF16),
            pltpu.VMEM((GROUPS, OWN, GCOLS), BF16),
            pltpu.VMEM((GROUPS, OWN, GCOLS), BF16),
            pltpu.VMEM((2 * OWN, GCOLS), F32),
            pltpu.VMEM((GROUPS, OWN, GCOLS), F32),
            dma((5,)),
            dma((4, 16, 2)),
            dma((4,)),
            dma((4,)),
            dma((5, GROUPS)),
            dma((5, GROUPS)),
        ],
        compiler_params=pltpu.CompilerParams(
            collective_id=0, has_side_effects=True, vmem_limit_bytes=66 * 1000 * 1000
        ),
    )(
        hidden, norm_gain.reshape(1, D), w_query, w_key, w_value, bias_query.reshape(1, 512),
        bias_key.reshape(1, 128), bias_value.reshape(1, 128), w_out, cs, sn,
    )


def solution(mesh):
    in_specs = (
        P("seq", None),
        P(),
        P("seq", "head"),
        P("seq", "head"),
        P("seq", "head"),
        P("head"),
        P("head"),
        P("head"),
        P("head", "seq"),
    )
    out_specs = P(("seq", "head"), None)
    return jax.shard_map(local, mesh=mesh, in_specs=in_specs, out_specs=out_specs, check_vma=False)
```

```python
import functools

import jax
import jax.numpy as jnp
from jax import lax
from jax.experimental import pallas as pl
from jax.experimental.pallas import tpu as pltpu
from jax.sharding import PartitionSpec as P

HEAD_DIM = 128
ROPE_BASE = 1000000.0
EPSILON = 1e-06
BF16 = jnp.bfloat16
F32 = jnp.float32
MESH = pl.DeviceIdType.MESH
ZS = 8
YS = 4
SEQ = 32
ROWS = 288
D = 8192
OWN = 36
GROUPS = 5
COLS = (1024, 2048, 2048, 2048, 1024)
BASE = (0, 1024, 3072, 5120, 7168)
KBLOCK = 1152
PADROWS = 80
SCALE2 = HEAD_DIM**-0.5 * 1.4426950408889634


def wrap(value, size):
    return lax.rem(value + size, size)


class Gather:
    def __init__(self, kind, buf, rows, place, recv, sib_sem, send_sem):
        self.kind, self.buf, self.rows, self.half = kind, buf, rows, rows // 2
        self.x, self.z, self.c, self.head = place
        self.recv, self.sib_sem, self.send_sem = recv, sib_sem, send_sem
        self.zp = self.at(self.x, 1)
        self.zm = self.at(self.x, -1)
        self.xp = self.at(1 - self.x, 0)
        self.sib = (self.x * ZS + self.z) * 2 + 1 - self.c

    def at(self, x, dz):
        return (x * ZS + wrap(self.z + dz, ZS)) * 2 + self.c

    def copy(self, s, part, dev, sem):
        ref = self.buf.at[pl.ds(pl.multiple_of(s * self.rows + part * self.half, 16), self.half)]
        return pltpu.make_async_remote_copy(
            src_ref=ref,
            dst_ref=ref,
            send_sem=self.send_sem.at[self.kind],
            recv_sem=sem,
            device_id=(dev, self.head),
            device_id_type=MESH,
        )

    def sem(self, s, part):
        return self.recv.at[self.kind, lax.div(s, 2), part]

    def send(self, k, s, part, *devs):
        for dev in devs:
            self.copy(s, part, dev, self.sem(s, part)).start()
        self.copy(s, part, self.sib, self.sib_sem.at[self.kind, k]).start()

    def relay(self, k, s, part, *devs):
        self.copy(s, part, self.sib, self.sem(s, part)).wait_recv()
        self.send(k, s, part, *devs)

    def own(self):
        s = self.at(self.x, 0)
        for part in (0, 1):
            self.send(0, s, part, self.zp, self.zm, self.xp)

    def cross(self):
        s = self.at(1 - self.x, 0)
        self.relay(0, s, 0, self.zp, self.zm)
        self.relay(0, s, 1)

    def step_a(self, k):
        self.relay(k, self.at(self.x, -k), 0, self.zp)
        self.relay(k, self.at(self.x, k), 0, self.zm)

    def step_b(self, k):
        self.relay(k, self.at(self.x, -k), 1, self.zp, self.xp)
        self.relay(k, self.at(self.x, k), 1, self.zm, self.xp)

    def step_c(self, k):
        self.relay(k, self.at(1 - self.x, -k), 0, self.zp)
        self.relay(k, self.at(1 - self.x, k), 0, self.zm)

    def step(self, k):
        self.step_a(k)
        self.step_b(k)
        self.step_c(k)

    def crossed(self, k):
        self.relay(k, self.at(1 - self.x, -k), 1)
        self.relay(k, self.at(1 - self.x, k), 1)

    def step3(self):
        lo, hi = self.at(self.x, -3), self.at(self.x, 3)
        self.relay(3, lo, 0, self.zp)
        self.relay(3, hi, 1, self.zm, self.xp)
        self.relay(3, lo, 1, self.xp)
        self.relay(3, hi, 0)
        self.relay(3, self.at(1 - self.x, -3), 0)
        self.relay(3, self.at(1 - self.x, 3), 0)

    def step4(self):
        far = self.at(self.x, 4)
        self.relay(4, far, 0, self.xp)
        self.relay(4, far, 1, self.xp)

    def last(self):
        far = self.at(1 - self.x, 4)
        self.relay(4, far, 0)
        self.relay(4, far, 1)

    def sibling(self, k):
        part = self.buf.at[pl.ds(0, (2 if k in (0, 4) else 4) * self.rows)]
        pltpu.make_async_copy(part, part, self.sib_sem.at[self.kind, k]).wait()

    def finish(self):
        for k in range(5):
            self.sibling(k)

    def drain(self):
        part = self.buf.at[pl.ds(0, 31 * self.rows)]
        pltpu.make_async_copy(part, part, self.send_sem.at[self.kind]).wait()


def rotated(values, cs, sn):
    return values * cs + pltpu.roll(values, HEAD_DIM // 2, 1) * sn


def kernel(
    hidden, gain, wq_in, wk_in, wv_in, bq, bk, bv, wo_in, cs, sn, out,
    hid, wkv, wq, kv, wo, qacc, qs, tmp, att32, att, terms, r1, r2, xs, xr, tot, keep,
    scores0, scores1, high, acc,
    local, recv, sib_sem, send_sem, rsem, r_send,
):
    s = lax.axis_index("seq")
    head = lax.axis_index("head")
    c = lax.rem(s, 2)
    chip = lax.div(s, 2)
    z = lax.rem(chip, ZS)
    x = lax.div(chip, ZS)
    y = lax.rem(head, YS)
    xh = lax.div(head, YS)
    place = (x, z, c, head)
    gather = functools.partial(Gather, place=place, recv=recv, sib_sem=sib_sem, send_sem=send_sem)
    g_kv_w = gather(0, wkv, 256)
    g_q_w = gather(1, wq, 256)
    g_kv = gather(2, kv, ROWS)
    g_o_w = gather(3, wo, 512)
    yp = xh * YS + wrap(y + 1, YS)
    ym = xh * YS + wrap(y - 1, YS)
    xhp = (1 - xh) * YS + y

    mine = pl.ds(pl.multiple_of(s * 256, 256), 256)
    mine_o = pl.ds(pl.multiple_of(s * 512, 512), 512)
    copies = [
        pltpu.make_async_copy(wk_in, wkv.at[mine, pl.ds(0, 128)], local.at[0]),
        pltpu.make_async_copy(wv_in, wkv.at[mine, pl.ds(128, 128)], local.at[1]),
        pltpu.make_async_copy(wq_in, wq.at[mine], local.at[2]),
        pltpu.make_async_copy(hidden, hid, local.at[3]),
        pltpu.make_async_copy(wo_in, wo.at[mine_o], local.at[4]),
    ]
    for copy in copies:
        copy.start()
    barrier = pltpu.get_barrier_semaphore()
    for dev in (g_q_w.zp, g_q_w.zm, g_q_w.xp, g_q_w.sib):
        pl.semaphore_signal(barrier, inc=1, device_id=(dev, head), device_id_type=MESH)
    for dev in (yp, ym, xhp):
        pl.semaphore_signal(barrier, inc=1, device_id=(s, dev), device_id_type=MESH)
    copies[0].wait()
    copies[1].wait()
    copies[2].wait()
    pl.semaphore_wait(barrier, 7)
    g_kv_w.own()
    g_q_w.own()

    copies[3].wait()

    @pl.loop(0, ROWS // 16)
    def _(i):
        rows = pl.ds(pl.multiple_of(i * 16, 16), 16)
        squares = jnp.zeros((16, 1024), F32)
        for j in range(8):
            part = hid[rows, pl.ds(j * 1024, 1024)].astype(F32)
            squares = squares + part * part
        inverse = lax.rsqrt(jnp.sum(squares, axis=-1, keepdims=True) * (1.0 / D) + EPSILON)
        for j in range(8):
            cols = pl.ds(j * 1024, 1024)
            part = hid[rows, cols].astype(F32)
            hid[rows, cols] = (part * inverse * gain[:, cols].astype(F32)).astype(BF16)

    def stages(g):
        g.step3()
        g.crossed(2)
        g.step4()
        g.crossed(3)
        g.last()

    g_kv_w.cross()
    g_kv_w.step(1)
    g_q_w.cross()
    g_kv_w.step(2)
    g_kv_w.crossed(1)
    g_q_w.step(1)
    stages(g_kv_w)
    g_kv_w.finish()

    def project(weights, cols):
        acc = qacc.at[:, pl.ds(0, cols)]
        acc[...] = jnp.zeros((ROWS, cols), F32)

        @pl.loop(0, 4)
        def _(i):
            depth = pl.ds(pl.multiple_of(i * 2048, 2048), 2048)
            acc[...] += jnp.dot(hid[:, depth], weights[depth, :], preferred_element_type=F32)

    project(wkv, 256)
    own_kv = pl.ds(pl.multiple_of(s * ROWS, 16), ROWS)
    kv[own_kv, 0:128] = rotated(qacc[:, 0:128] + bk[...].astype(F32), cs[...], sn[...]).astype(BF16)
    kv[own_kv, 128:256] = (qacc[:, 128:256] + bv[...].astype(F32)).astype(BF16)
    g_q_w.step(2)
    g_kv.own()
    g_q_w.crossed(1)
    g_kv.cross()
    g_q_w.step3()
    g_q_w.crossed(2)
    g_kv.step(1)
    g_q_w.step4()
    g_kv.step(2)
    g_kv.crossed(1)
    g_q_w.crossed(3)
    copies[4].wait()
    g_o_w.own()
    g_q_w.last()
    g_kv.step3()
    g_kv.crossed(2)
    g_q_w.finish()
    project(wq, 512)
    for j in range(4):
        cols = pl.ds(j * HEAD_DIM, HEAD_DIM)
        value = qacc[:, cols] + bq[:, cols].astype(F32)
        qs[pl.ds(j * ROWS, ROWS), :] = rotated(value, cs[...], sn[...]).astype(BF16)
    g_kv.step4()
    g_kv.crossed(3)
    g_kv.last()
    g_o_w.cross()
    g_kv.finish()

    last_block = lax.div(s, 4)
    score_bufs = (scores0, scores1)

    def set_scores(j, block):
        keys = kv[pl.ds(pl.multiple_of(block * KBLOCK, KBLOCK), KBLOCK), 0:128]
        score_bufs[j % 2][...] = lax.dot_general(
            qs[pl.ds(j * ROWS, ROWS), :], keys, (((1,), (1,)), ((), ())), preferred_element_type=F32
        )

    def attend(block, following, diagonal):
        values = kv[pl.ds(pl.multiple_of(block * KBLOCK, KBLOCK), KBLOCK), 128:256]
        weights = jnp.concatenate([values, jnp.ones((KBLOCK, HEAD_DIM), BF16)], axis=1)
        for j in range(4):
            rows = pl.ds(j * ROWS, ROWS)
            set_scores((j + 1) % 4, block if j < 3 else following)
            scores = score_bufs[j % 2][...]
            if diagonal:
                query_pos = s * ROWS + lax.broadcasted_iota(jnp.int32, (ROWS, KBLOCK), 0)
                key_pos = block * KBLOCK + lax.broadcasted_iota(jnp.int32, (ROWS, KBLOCK), 1)
                scores = jnp.where(query_pos >= key_pos, scores, -jnp.inf)
            new_high = jnp.broadcast_to(jnp.max(scores, axis=-1, keepdims=True), (ROWS, HEAD_DIM))
            if not diagonal:
                old_high = high[rows, :]
                new_high = jnp.maximum(old_high, new_high)
            probs = jnp.exp2((scores - jnp.tile(new_high, (1, KBLOCK // HEAD_DIM))) * SCALE2)
            mixed = jnp.dot(probs.astype(BF16), weights, preferred_element_type=F32)
            if not diagonal:
                fade = jnp.exp2((old_high - new_high) * SCALE2)
                mixed = acc[rows, :] * jnp.tile(fade, (1, 2)) + mixed
            acc[rows, :] = mixed
            high[rows, :] = new_high

    set_scores(0, last_block)
    attend(last_block, 0, True)
    relays = (
        lambda: g_o_w.step_a(1),
        lambda: g_o_w.step_b(1),
        lambda: g_o_w.step_c(1),
        lambda: g_o_w.step_a(2),
        lambda: g_o_w.step_b(2),
        lambda: g_o_w.step_c(2),
        lambda: g_o_w.crossed(1),
    )

    @pl.loop(0, 7)
    def _(block):
        @pl.when(block < last_block)
        def _():
            attend(block, block + 1, False)

        for k, relay in enumerate(relays):
            pl.when(block == k)(relay)

    att32[...] = jnp.zeros(att32.shape, F32)
    for j in range(4):
        rows = pl.ds(j * ROWS, ROWS)
        tmp[...] = acc[rows, 0:HEAD_DIM] / acc[rows, HEAD_DIM : 2 * HEAD_DIM]
        for h in range(8):
            spot = PADROWS * (h % YS) + OWN * (h // YS)
            att32[pl.ds(spot, OWN), pl.ds(j * HEAD_DIM, HEAD_DIM)] = tmp[pl.ds(h * OWN, OWN), :]
    att[...] = att32[...].astype(BF16)

    y2 = wrap(y + 2, YS)
    y_next = wrap(y + 1, YS)
    y_prev = wrap(y - 1, YS)

    def move(src, dst, kind, g, dev):
        return pltpu.make_async_remote_copy(
            src_ref=src,
            dst_ref=dst,
            send_sem=r_send.at[kind, g],
            recv_sem=rsem.at[kind, g],
            device_id=(s, dev),
            device_id_type=MESH,
        )

    def first(g, kind):
        half = COLS[g] // 2
        cols = pl.ds(BASE[g] + kind * half, half)
        near = r1.at[kind, :, pl.ds(BASE[g] // 2, half)]
        return move(terms.at[y2, :, cols], near, kind, g, ym if kind else yp)

    def second(g, kind):
        cols = pl.ds(BASE[g], COLS[g])
        row = y_prev if kind else y_next
        return move(terms.at[row, :, cols], r2.at[kind, :, cols], 2 + kind, g, ym if kind else yp)

    def third(g):
        cols = pl.ds(BASE[g], COLS[g])
        return move(xs.at[:, cols], xr.at[:, cols], 4, g, xhp)

    def slot_of(g, i):
        ends = g in (0, 4)
        other = lax.div(i, 2 if ends else 4)
        side = 0 if ends else lax.rem(lax.div(i, 2), 2)
        core = lax.rem(i, 2)
        xx = x + other - 2 * x * other
        return (xx * ZS + wrap(z + g - 2 * g * side, ZS)) * 2 + c + core - 2 * c * core

    def compute(g):
        g_o_w.sibling(g)

        @pl.loop(0, COLS[g] // 256)
        def _(i):
            depth = pl.ds(pl.multiple_of(slot_of(g, i) * 512, 512), 512)
            cols = pl.ds(pl.multiple_of(BASE[g] + i * 256, 256), 256)
            term = jnp.dot(att[...], wo[depth, :], preferred_element_type=F32).astype(BF16)
            for k in range(YS):
                terms[k, :, cols] = term[PADROWS * k : PADROWS * k + 2 * OWN]

        first(g, 0).start()
        first(g, 1).start()

    def pair(g):
        for kind in (0, 1):
            first(g, kind).wait_recv()
            row = y_prev if kind else y_next
            half = COLS[g] // 2
            cols = pl.ds(BASE[g] + kind * half, half)
            near = r1[kind, :, pl.ds(BASE[g] // 2, half)].astype(F32)
            terms[row, :, cols] = (terms[row, :, cols].astype(F32) + near).astype(BF16)
            second(g, kind).start()

    def across(g):
        second(g, 0).wait_recv()
        second(g, 1).wait_recv()
        cols = pl.ds(BASE[g], COLS[g])
        part = tot.at[:, pl.ds(0, COLS[g])]
        part[...] = terms[y, :, cols].astype(F32) + r2[0, :, cols].astype(F32) + r2[1, :, cols].astype(F32)
        low, high_rows = part[0:OWN, :], part[OWN : 2 * OWN, :]
        lower = xh == 0
        xs[:, cols] = jnp.where(lower, high_rows, low).astype(BF16)
        keep[:, cols] = jnp.where(lower, low, high_rows)
        third(g).start()

    def done(g):
        third(g).wait_recv()

        @pl.loop(0, COLS[g] // 256)
        def _(i):
            cols = pl.ds(pl.multiple_of(BASE[g] + i * 256, 256), 256)
            there = pl.ds(pl.multiple_of(slot_of(g, i) * 256, 256), 256)
            out[:, there] = (keep[:, cols] + xr[:, cols].astype(F32)).astype(BF16)

    compute(0)
    compute(1)
    pair(0)
    g_o_w.step3()
    g_o_w.crossed(2)
    compute(2)
    pair(1)
    across(0)
    g_o_w.step4()
    g_o_w.crossed(3)
    compute(3)
    pair(2)
    g_o_w.last()
    compute(4)
    across(1)
    done(0)
    pair(3)
    pair(4)
    across(2)
    done(1)
    across(3)
    across(4)
    done(2)
    done(3)
    done(4)

    for g in range(GROUPS):
        for kind in (0, 1):
            first(g, kind).wait_send()
            second(g, kind).wait_send()
        third(g).wait_send()
    for g in (g_kv_w, g_q_w, g_kv, g_o_w):
        g.drain()


def local(hidden, norm_gain, w_query, w_key, w_value, bias_query, bias_key, bias_value, w_out):
    first_row = lax.axis_index("seq") * ROWS
    positions = first_row + jnp.arange(ROWS, dtype=jnp.int32)
    half_dim = HEAD_DIM // 2
    freq = ROPE_BASE ** (-2.0 * jnp.arange(half_dim, dtype=F32) / HEAD_DIM)
    angles = positions.astype(F32)[:, None] * freq[None, :]
    cosine, sine = jnp.cos(angles), jnp.sin(angles)
    cs = jnp.concatenate([cosine, cosine], axis=-1)
    sn = jnp.concatenate([-sine, sine], axis=-1)
    vmem = pl.BlockSpec(memory_space=pltpu.VMEM)
    hbm = pl.BlockSpec(memory_space=pl.ANY)
    dma = pltpu.SemaphoreType.DMA
    return pl.pallas_call(
        kernel,
        name="layer",
        out_shape=jax.ShapeDtypeStruct((OWN, D), BF16),
        in_specs=[hbm, vmem, hbm, hbm, hbm, vmem, vmem, vmem, hbm, vmem, vmem],
        out_specs=vmem,
        scratch_shapes=[
            pltpu.VMEM((ROWS, D), BF16),
            pltpu.VMEM((D, 256), BF16),
            pltpu.VMEM((D, 512), BF16),
            pltpu.VMEM((SEQ * ROWS, 256), BF16),
            pltpu.VMEM((SEQ * 512, 256), BF16),
            pltpu.VMEM((ROWS, 512), F32),
            pltpu.VMEM((4 * ROWS, HEAD_DIM), BF16),
            pltpu.VMEM((ROWS, HEAD_DIM), F32),
            pltpu.VMEM((YS * PADROWS, 512), F32),
            pltpu.VMEM((YS * PADROWS, 512), BF16),
            pltpu.VMEM((YS, 2 * OWN, D), BF16),
            pltpu.VMEM((2, 2 * OWN, D // 2), BF16),
            pltpu.VMEM((2, 2 * OWN, D), BF16),
            pltpu.VMEM((OWN, D), BF16),
            pltpu.VMEM((OWN, D), BF16),
            pltpu.VMEM((2 * OWN, 2048), F32),
            pltpu.VMEM((OWN, D), F32),
            pltpu.VMEM((ROWS, KBLOCK), F32),
            pltpu.VMEM((ROWS, KBLOCK), F32),
            pltpu.VMEM((4 * ROWS, HEAD_DIM), F32),
            pltpu.VMEM((4 * ROWS, 2 * HEAD_DIM), F32),
            dma((5,)),
            dma((4, 16, 2)),
            dma((4, 5)),
            dma((4,)),
            dma((5, GROUPS)),
            dma((5, GROUPS)),
        ],
        compiler_params=pltpu.CompilerParams(
            collective_id=0, has_side_effects=True, vmem_limit_bytes=66 * 1000 * 1000
        ),
    )(
        hidden, norm_gain.reshape(1, D), w_query, w_key, w_value, bias_query.reshape(1, 512),
        bias_key.reshape(1, 128), bias_value.reshape(1, 128), w_out, cs, sn,
    )


def solution(mesh):
    in_specs = (
        P("seq", None),
        P(),
        P("seq", "head"),
        P("seq", "head"),
        P("seq", "head"),
        P("head"),
        P("head"),
        P("head"),
        P("head", "seq"),
    )
    out_specs = P(("seq", "head"), None)
    return jax.shard_map(local, mesh=mesh, in_specs=in_specs, out_specs=out_specs, check_vma=False)
```

```python
import functools

import jax
import jax.numpy as jnp
import numpy as np
from jax import lax
from jax.experimental import pallas as pl
from jax.experimental.pallas import tpu as pltpu
from jax.sharding import PartitionSpec as P

HEAD_DIM = 128
ROPE_BASE = 1000000.0
EPSILON = 1e-06
BF16 = jnp.bfloat16
F32 = jnp.float32
MESH = pl.DeviceIdType.MESH
ZS = 8
YS = 4
SEQ = 32
ROWS = 288
D = 8192
OWN = 36
GROUPS = 5
COLS = (1024, 2048, 2048, 2048, 1024)
BASE = (0, 1024, 3072, 5120, 7168)
KBLOCK = 1152
PADROWS = 80
BEFORE = (
    ("own", "k"),
    ("own", "q"),
    ("norm", 0),
    ("cross", "k"),
    ("a", "k", 1),
    ("norm", 1),
    ("b", "k", 1),
    ("c", "k", 1),
    ("norm", 2),
    ("a", "k", 2),
    ("norm", 3),
    ("b", "k", 2),
    ("c", "k", 2),
    ("norm", 4),
    ("cross", "q"),
    ("x", "k", 1),
    ("a", "q", 1),
    ("s3", "k"),
    ("norm", 5),
    ("pk", 0),
    ("b", "q", 1),
    ("c", "q", 1),
    ("x", "k", 2),
    ("s4", "k"),
    ("a", "q", 2),
    ("x", "k", 3),
    ("pk", 1),
    ("pk", 2),
    ("b", "q", 2),
    ("last", "k"),
    ("c", "q", 2),
    ("pk", 3),
    ("pk", 4),
    ("ropek",),
    ("own", "v"),
    ("x", "q", 1),
    ("s3", "q"),
    ("x", "q", 2),
    ("pq", 0),
    ("cross", "v"),
    ("a", "v", 1),
    ("pq", 1),
    ("b", "v", 1),
    ("pq", 2),
    ("s4", "q"),
    ("c", "v", 1),
    ("a", "v", 2),
    ("b", "v", 2),
    ("c", "v", 2),
    ("x", "q", 3),
    ("last", "q"),
    ("own", "o"),
    ("x", "v", 1),
    ("pq", 3),
    ("s3", "v"),
    ("pq", 4),
    ("ropeq",),
    ("x", "v", 2),
)
BETWEEN = (
    (),
    (("cross", "o"), ("a", "o", 1), ),
    (("s4", "v"), ("x", "v", 3), ("b", "o", 1), ),
    (("c", "o", 1), ),
    (("last", "v"), ("a", "o", 2), ),
    (("b", "o", 2), ),
    (("c", "o", 2), ("x", "o", 1), ),
)
AFTER = (
    ("fin",),
    ("comp", 0),
    ("comp", 1),
    ("s3", "o"),
    ("x", "o", 2),
    ("pair", 0),
    ("pair", 1),
    ("s4", "o"),
    ("comp", 2),
    ("x", "o", 3),
    ("comp", 3),
    ("across", 0),
    ("last", "o"),
    ("comp", 4),
    ("pair", 2),
    ("across", 1),
    ("pair", 3),
    ("across", 2),
    ("pair", 4),
    ("done", 0),
    ("done", 1),
    ("across", 3),
    ("across", 4),
    ("done", 2),
    ("done", 3),
    ("done", 4),
)
SCALE2 = HEAD_DIM**-0.5 * 1.4426950408889634


def wrap(value, size):
    return lax.rem(value + size, size)


class Gather:
    def __init__(self, kind, buf, rows, place, recv, sib_sem, send_sem):
        self.kind, self.buf, self.rows, self.half = kind, buf, rows, rows // 2
        self.x, self.z, self.c, self.head = place
        self.recv, self.sib_sem, self.send_sem = recv, sib_sem, send_sem
        self.zp = self.at(self.x, 1)
        self.zm = self.at(self.x, -1)
        self.xp = self.at(1 - self.x, 0)
        self.sib = (self.x * ZS + self.z) * 2 + 1 - self.c

    def at(self, x, dz):
        return (x * ZS + wrap(self.z + dz, ZS)) * 2 + self.c

    def copy(self, s, part, dev, sem):
        ref = self.buf.at[pl.ds(pl.multiple_of(s * self.rows + part * self.half, 16), self.half)]
        return pltpu.make_async_remote_copy(
            src_ref=ref,
            dst_ref=ref,
            send_sem=self.send_sem.at[self.kind],
            recv_sem=sem,
            device_id=(dev, self.head),
            device_id_type=MESH,
        )

    def sem(self, s, part):
        return self.recv.at[self.kind, lax.div(s, 2), part]

    def send(self, k, other, s, part, *devs):
        for dev in devs:
            self.copy(s, part, dev, self.sem(s, part)).start()
        self.copy(s, part, self.sib, self.sib_sem.at[self.kind, k + 5 * other]).start()

    def relay(self, k, other, dz, part, *devs):
        s = self.at(1 - self.x if other else self.x, dz)
        self.copy(s, part, self.sib, self.sem(s, part)).wait_recv()
        self.send(k, other, s, part, *devs)

    def own(self):
        for part in (0, 1):
            self.send(0, 0, self.at(self.x, 0), part, self.zp, self.zm, self.xp)

    def cross(self):
        self.relay(0, 1, 0, 0, self.zp, self.zm)
        self.relay(0, 1, 0, 1)

    def a(self, k):
        self.relay(k, 0, -k, 0, self.zp)
        self.relay(k, 0, k, 0, self.zm)

    def b(self, k):
        self.relay(k, 0, -k, 1, self.zp, self.xp)
        self.relay(k, 0, k, 1, self.zm, self.xp)

    def c2(self, k):
        self.relay(k, 1, -k, 0, self.zp)
        self.relay(k, 1, k, 0, self.zm)

    def x2(self, k):
        self.relay(k, 1, -k, 1)
        self.relay(k, 1, k, 1)

    def s3(self):
        self.relay(3, 0, -3, 0, self.zp)
        self.relay(3, 0, 3, 1, self.zm, self.xp)
        self.relay(3, 0, -3, 1, self.xp)
        self.relay(3, 0, 3, 0)
        self.relay(3, 1, -3, 0)
        self.relay(3, 1, 3, 0)

    def s4(self):
        self.relay(4, 0, 4, 0, self.xp)
        self.relay(4, 0, 4, 1, self.xp)

    def last(self):
        self.relay(4, 1, 4, 0)
        self.relay(4, 1, 4, 1)

    def sibling(self, k, *others):
        for other in others:
            part = self.buf.at[pl.ds(0, (1 if k in (0, 4) else 2) * self.rows)]
            pltpu.make_async_copy(part, part, self.sib_sem.at[self.kind, k + 5 * other]).wait()

    def drain(self):
        part = self.buf.at[pl.ds(0, 31 * self.rows)]
        pltpu.make_async_copy(part, part, self.send_sem.at[self.kind]).wait()


def rotated(values, cs, sn):
    return values * cs + pltpu.roll(values, HEAD_DIM // 2, 1) * sn


def kernel(
    hidden, vecs, wq_in, wk_in, wv_in, wo_in, table, out,
    hid, wkv, wq, kv, wo, kacc, qacc, qs, cs, sn, tmp, att32, att, terms, r1, r2, xs, xr, tot, keep,
    scores0, scores1, high, acc, local, recv, sib_sem, send_sem, rsem, r_send,
):
    s = lax.axis_index("seq")
    head = lax.axis_index("head")
    c = lax.rem(s, 2)
    chip = lax.div(s, 2)
    z = lax.rem(chip, ZS)
    x = lax.div(chip, ZS)
    y = lax.rem(head, YS)
    xh = lax.div(head, YS)
    place = (x, z, c, head)
    gather = functools.partial(Gather, place=place, recv=recv, sib_sem=sib_sem, send_sem=send_sem)
    g_kv_w = gather(0, wkv, 256)
    g_q_w = gather(1, wq, 256)
    g_kv = gather(2, kv, ROWS)
    g_o_w = gather(3, wo, 512)
    yp = xh * YS + wrap(y + 1, YS)
    ym = xh * YS + wrap(y - 1, YS)
    xhp = (1 - xh) * YS + y

    mine = pl.ds(pl.multiple_of(s * 256, 256), 256)
    mine_o = pl.ds(pl.multiple_of(s * 512, 512), 512)
    copies = [
        pltpu.make_async_copy(wk_in, wkv.at[mine, pl.ds(0, 128)], local.at[0]),
        pltpu.make_async_copy(wv_in, wkv.at[mine, pl.ds(128, 128)], local.at[1]),
        pltpu.make_async_copy(wq_in, wq.at[mine], local.at[2]),
        pltpu.make_async_copy(hidden, hid, local.at[3]),
        pltpu.make_async_copy(wo_in, wo.at[mine_o], local.at[4]),
    ]
    for copy in copies:
        copy.start()
    barrier = pltpu.get_barrier_semaphore()
    for dev in (g_q_w.zp, g_q_w.zm, g_q_w.xp, g_q_w.sib):
        pl.semaphore_signal(barrier, inc=1, device_id=(dev, head), device_id_type=MESH)
    for dev in (yp, ym, xhp):
        pl.semaphore_signal(barrier, inc=1, device_id=(s, dev), device_id_type=MESH)
    copies[0].wait()
    copies[1].wait()
    copies[2].wait()
    pl.semaphore_wait(barrier, 7)
    kinds = {"k": g_kv_w, "q": g_q_w, "v": g_kv, "o": g_o_w}

    def norm(chunk):
        if chunk == 0:
            copies[3].wait()

        @pl.loop(3 * chunk, 3 * chunk + 3)
        def _(i):
            rows = pl.ds(pl.multiple_of(i * 16, 16), 16)
            squares = jnp.zeros((16, 1024), F32)
            for j in range(8):
                part = hid[rows, pl.ds(j * 1024, 1024)].astype(F32)
                squares = squares + part * part
            inverse = lax.rsqrt(jnp.sum(squares, axis=-1, keepdims=True) * (1.0 / D) + EPSILON)
            for j in range(8):
                cols = pl.ds(j * 1024, 1024)
                part = hid[rows, cols].astype(F32)
                hid[rows, cols] = (part * inverse * vecs[:, cols]).astype(BF16)

    def tables():
        cos_row, sin_row = table[0:ROWS, :], table[ROWS : 2 * ROWS, :]
        cos_first = table[pl.ds(2 * ROWS + s, 1), :]
        sin_first = table[pl.ds(2 * ROWS + SEQ + s, 1), :]
        cs[...] = cos_first * cos_row - sin_first * sin_row
        sine = sin_first * cos_row + cos_first * sin_row
        lane = lax.broadcasted_iota(jnp.int32, (ROWS, HEAD_DIM), 1)
        sn[...] = jnp.where(lane < HEAD_DIM // 2, -sine, sine)

    def project(gather, sums, k):
        gather.sibling(k, 0, 1)
        total = None
        for other in (0, 1):
            for dz in (0,) if k == 0 else (4,) if k == 4 else (-k, k):
                place = lax.div(gather.at(1 - x if other else x, dz), 2)
                depth = pl.ds(pl.multiple_of(place * 512, 512), 512)
                term = jnp.dot(hid[:, depth], gather.buf[depth, :], preferred_element_type=F32)
                total = term if total is None else total + term
        sums[...] = total if k == 0 else sums[...] + total

    def store_kv():
        own_kv = pl.ds(pl.multiple_of(s * ROWS, 16), ROWS)
        bk = vecs[:, D + 512 : D + 640]
        bv = vecs[:, D + 640 : D + 768]
        kv[own_kv, 0:128] = rotated(kacc[:, 0:128] + bk, cs[...], sn[...]).astype(BF16)
        kv[own_kv, 128:256] = (kacc[:, 128:256] + bv).astype(BF16)

    def store_q():
        for j in range(4):
            cols = pl.ds(j * HEAD_DIM, HEAD_DIM)
            value = qacc[:, cols] + vecs[:, pl.ds(D + j * HEAD_DIM, HEAD_DIM)]
            qs[pl.ds(j * ROWS, ROWS), :] = rotated(value, cs[...], sn[...]).astype(BF16)

    last_block = lax.div(s, 4)
    score_bufs = (scores0, scores1)

    def set_scores(j, block):
        keys = kv[pl.ds(pl.multiple_of(block * KBLOCK, KBLOCK), KBLOCK), 0:128]
        score_bufs[j % 2][...] = lax.dot_general(
            qs[pl.ds(j * ROWS, ROWS), :], keys, (((1,), (1,)), ((), ())), preferred_element_type=F32
        )

    def attend(block, following, diagonal):
        values = kv[pl.ds(pl.multiple_of(block * KBLOCK, KBLOCK), KBLOCK), 128:256]
        weights = jnp.concatenate([values, jnp.ones((KBLOCK, HEAD_DIM), BF16)], axis=1)
        for j in range(4):
            rows = pl.ds(j * ROWS, ROWS)
            set_scores((j + 1) % 4, block if j < 3 else following)
            scores = score_bufs[j % 2][...]
            if diagonal:
                query_pos = s * ROWS + lax.broadcasted_iota(jnp.int32, (ROWS, KBLOCK), 0)
                key_pos = block * KBLOCK + lax.broadcasted_iota(jnp.int32, (ROWS, KBLOCK), 1)
                scores = jnp.where(query_pos >= key_pos, scores, -jnp.inf)
            new_high = jnp.broadcast_to(jnp.max(scores, axis=-1, keepdims=True), (ROWS, HEAD_DIM))
            if not diagonal:
                old_high = high[rows, :]
                new_high = jnp.maximum(old_high, new_high)
            probs = jnp.exp2((scores - jnp.tile(new_high, (1, KBLOCK // HEAD_DIM))) * SCALE2)
            mixed = jnp.dot(probs.astype(BF16), weights, preferred_element_type=F32)
            if not diagonal:
                fade = jnp.exp2((old_high - new_high) * SCALE2)
                mixed = acc[rows, :] * jnp.tile(fade, (1, 2)) + mixed
            acc[rows, :] = mixed
            high[rows, :] = new_high

    def block_at(i):
        own = (i < 3) | (i == 6)
        column = jnp.where(own, x, 1 - x)
        step = jnp.where(i >= 6, 2, jnp.where(i < 3, jnp.where(i == 2, 1, -i), jnp.where(i == 5, 1, 3 - i)))
        return 4 * column + lax.rem(lax.div(z, 2) + step + 4, 4)

    def arrived(i):
        for k, other in {0: ((0, 0), (1, 0), (2, 0), (3, 0)), 2: ((0, 1), (1, 1)), 3: ((2, 1), (3, 1)), 5: ((4, 0),), 6: ((4, 1),)}.get(i, ()):
            g_kv.sibling(k, other)

    def finish_attention():
        att32[...] = jnp.zeros(att32.shape, F32)
        for j in range(4):
            rows = pl.ds(j * ROWS, ROWS)
            tmp[...] = acc[rows, 0:HEAD_DIM] / acc[rows, HEAD_DIM : 2 * HEAD_DIM]
            for h in range(8):
                spot = PADROWS * (h % YS) + OWN * (h // YS)
                att32[pl.ds(spot, OWN), pl.ds(j * HEAD_DIM, HEAD_DIM)] = tmp[pl.ds(h * OWN, OWN), :]
        att[...] = att32[...].astype(BF16)

    y2 = wrap(y + 2, YS)
    y_next = wrap(y + 1, YS)
    y_prev = wrap(y - 1, YS)

    def move(src, dst, kind, g, dev):
        return pltpu.make_async_remote_copy(
            src_ref=src,
            dst_ref=dst,
            send_sem=r_send.at[kind, g],
            recv_sem=rsem.at[kind, g],
            device_id=(s, dev),
            device_id_type=MESH,
        )

    def first(g, kind):
        half = COLS[g] // 2
        cols = pl.ds(BASE[g] + kind * half, half)
        near = r1.at[kind, :, pl.ds(BASE[g] // 2, half)]
        return move(terms.at[y2, :, cols], near, kind, g, ym if kind else yp)

    def second(g, kind):
        cols = pl.ds(BASE[g], COLS[g])
        row = y_prev if kind else y_next
        return move(terms.at[row, :, cols], r2.at[kind, :, cols], 2 + kind, g, ym if kind else yp)

    def third(g):
        cols = pl.ds(BASE[g], COLS[g])
        return move(xs.at[:, cols], xr.at[:, cols], 4, g, xhp)

    def slot_of(g, i):
        ends = g in (0, 4)
        other = lax.div(i, 2 if ends else 4)
        side = 0 if ends else lax.rem(lax.div(i, 2), 2)
        core = lax.rem(i, 2)
        xx = x + other - 2 * x * other
        return (xx * ZS + wrap(z + g - 2 * g * side, ZS)) * 2 + c + core - 2 * c * core

    def compute(g):
        g_o_w.sibling(g, 0, 1)

        @pl.loop(0, COLS[g] // 256)
        def _(i):
            depth = pl.ds(pl.multiple_of(slot_of(g, i) * 512, 512), 512)
            cols = pl.ds(pl.multiple_of(BASE[g] + i * 256, 256), 256)
            term = jnp.dot(att[...], wo[depth, :], preferred_element_type=F32).astype(BF16)
            for k in range(YS):
                terms[k, :, cols] = term[PADROWS * k : PADROWS * k + 2 * OWN]

        first(g, 0).start()
        first(g, 1).start()

    def pair(g):
        for kind in (0, 1):
            first(g, kind).wait_recv()
            row = y_prev if kind else y_next
            half = COLS[g] // 2
            cols = pl.ds(BASE[g] + kind * half, half)
            near = r1[kind, :, pl.ds(BASE[g] // 2, half)].astype(F32)
            terms[row, :, cols] = (terms[row, :, cols].astype(F32) + near).astype(BF16)
            second(g, kind).start()

    def across(g):
        second(g, 0).wait_recv()
        second(g, 1).wait_recv()
        cols = pl.ds(BASE[g], COLS[g])
        part = tot.at[:, pl.ds(0, COLS[g])]
        part[...] = terms[y, :, cols].astype(F32) + r2[0, :, cols].astype(F32) + r2[1, :, cols].astype(F32)
        low, high_rows = part[0:OWN, :], part[OWN : 2 * OWN, :]
        lower = xh == 0
        xs[:, cols] = jnp.where(lower, high_rows, low).astype(BF16)
        keep[:, cols] = jnp.where(lower, low, high_rows)
        third(g).start()

    def done(g):
        third(g).wait_recv()

        @pl.loop(0, COLS[g] // 256)
        def _(i):
            cols = pl.ds(pl.multiple_of(BASE[g] + i * 256, 256), 256)
            there = pl.ds(pl.multiple_of(slot_of(g, i) * 256, 256), 256)
            out[:, there] = (keep[:, cols] + xr[:, cols].astype(F32)).astype(BF16)

    def run(op):
        name, rest = op[0], op[1:]
        if name in ("own", "cross", "s3", "s4", "last"):
            if op == ("own", "o"):
                copies[4].wait()
            getattr(kinds[rest[0]], name)()
        elif name in ("a", "b"):
            getattr(kinds[rest[0]], name)(rest[1])
        elif name in ("c", "x"):
            getattr(kinds[rest[0]], name + "2")(rest[1])
        elif name == "pk":
            project(g_kv_w, kacc, rest[0])
        elif name == "pq":
            project(g_q_w, qacc, rest[0])
        else:
            simple[name](*rest)

    simple = {
        "norm": norm,
        "ropek": store_kv,
        "ropeq": store_q,
        "fin": finish_attention,
        "comp": compute,
        "pair": pair,
        "across": across,
        "done": done,
    }
    tables()
    for op in BEFORE:
        run(op)
    arrived(0)
    set_scores(0, last_block)
    attend(last_block, block_at(1), True)

    @pl.loop(1, 8)
    def _(i):
        for n, ops in enumerate(BETWEEN):

            @pl.when(i == n + 1)
            def _():
                for op in ops:
                    run(op)
                arrived(n + 1)

        block, following = block_at(i), block_at(jnp.minimum(i + 1, 7))

        @pl.when(block < last_block)
        def _():
            attend(block, following, False)

        @pl.when(block >= last_block)
        def _():
            set_scores(0, following)

    for op in AFTER:
        run(op)

    for g in range(GROUPS):
        for kind in (0, 1):
            first(g, kind).wait_send()
            second(g, kind).wait_send()
        third(g).wait_send()
    for g in (g_kv_w, g_q_w, g_kv, g_o_w):
        g.drain()


def rotary_table():
    half_dim = HEAD_DIM // 2
    freq = ROPE_BASE ** (-2.0 * np.arange(half_dim) / HEAD_DIM)
    rows = np.arange(ROWS)[:, None] * freq
    firsts = ROWS * np.arange(SEQ)[:, None] * freq
    parts = (np.cos(rows), np.sin(rows), np.cos(firsts), np.sin(firsts))
    return np.tile(np.concatenate(parts, axis=0), (1, 2)).astype(np.float32)


def local(hidden, norm_gain, w_query, w_key, w_value, bias_query, bias_key, bias_value, w_out):
    vecs = jnp.concatenate([norm_gain, bias_query, bias_key, bias_value]).astype(F32)
    vmem = pl.BlockSpec(memory_space=pltpu.VMEM)
    hbm = pl.BlockSpec(memory_space=pl.ANY)
    dma = pltpu.SemaphoreType.DMA
    return pl.pallas_call(
        kernel,
        name="layer",
        out_shape=jax.ShapeDtypeStruct((OWN, D), BF16),
        in_specs=[hbm, vmem, hbm, hbm, hbm, hbm, vmem],
        out_specs=vmem,
        scratch_shapes=[
            pltpu.VMEM((ROWS, D), BF16),
            pltpu.VMEM((D, 256), BF16),
            pltpu.VMEM((D, 512), BF16),
            pltpu.VMEM((SEQ * ROWS, 256), BF16),
            pltpu.VMEM((SEQ * 512, 256), BF16),
            pltpu.VMEM((ROWS, 256), F32),
            pltpu.VMEM((ROWS, 512), F32),
            pltpu.VMEM((4 * ROWS, HEAD_DIM), BF16),
            pltpu.VMEM((ROWS, HEAD_DIM), F32),
            pltpu.VMEM((ROWS, HEAD_DIM), F32),
            pltpu.VMEM((ROWS, HEAD_DIM), F32),
            pltpu.VMEM((YS * PADROWS, 512), F32),
            pltpu.VMEM((YS * PADROWS, 512), BF16),
            pltpu.VMEM((YS, 2 * OWN, D), BF16),
            pltpu.VMEM((2, 2 * OWN, D // 2), BF16),
            pltpu.VMEM((2, 2 * OWN, D), BF16),
            pltpu.VMEM((OWN, D), BF16),
            pltpu.VMEM((OWN, D), BF16),
            pltpu.VMEM((2 * OWN, 2048), F32),
            pltpu.VMEM((OWN, D), F32),
            pltpu.VMEM((ROWS, KBLOCK), F32),
            pltpu.VMEM((ROWS, KBLOCK), F32),
            pltpu.VMEM((4 * ROWS, HEAD_DIM), F32),
            pltpu.VMEM((4 * ROWS, 2 * HEAD_DIM), F32),
            dma((5,)),
            dma((4, 16, 2)),
            dma((4,10)),
            dma((4,)),
            dma((5, GROUPS)),
            dma((5, GROUPS)),
        ],
        compiler_params=pltpu.CompilerParams(
            collective_id=0, has_side_effects=True, vmem_limit_bytes=66 * 1000 * 1000
        ),
    )(hidden, vecs.reshape(1, -1), w_query, w_key, w_value, w_out, jnp.asarray(rotary_table()))


def solution(mesh):
    in_specs = (
        P("seq", None),
        P(),
        P("seq", "head"),
        P("seq", "head"),
        P("seq", "head"),
        P("head"),
        P("head"),
        P("head"),
        P("head", "seq"),
    )
    out_specs = P(("seq", "head"), None)
    return jax.shard_map(local, mesh=mesh, in_specs=in_specs, out_specs=out_specs, check_vma=False)
```

```python
import functools

import jax
import jax.numpy as jnp
import numpy as np
from jax import lax
from jax.experimental import pallas as pl
from jax.experimental.pallas import tpu as pltpu
from jax.sharding import PartitionSpec as P

HEAD_DIM = 128
ROPE_BASE = 1000000.0
EPSILON = 1e-06
BF16 = jnp.bfloat16
F32 = jnp.float32
MESH = pl.DeviceIdType.MESH
ZS = 8
YS = 4
SEQ = 32
ROWS = 288
D = 8192
OWN = 36
GROUPS = 5
COLS = (1024, 2048, 2048, 2048, 1024)
BASE = (0, 1024, 3072, 5120, 7168)
KBLOCK = 1152
PADROWS = 80
XBASE = {3: 0}
XCOLS = 2048
BEFORE = (
    ("own", "k"),
    ("norm", 0),
    ("own", "q"),
    ("cross", "k"),
    ("norm", 1),
    ("a", "k", 1),
    ("b", "k", 1),
    ("c", "k", 1),
    ("norm", 2),
    ("a", "k", 2),
    ("norm", 3),
    ("norm", 4),
    ("b", "k", 2),
    ("c", "k", 2),
    ("x", "k", 1),
    ("cross", "q"),
    ("norm", 5),
    ("a", "q", 1),
    ("s3", "k"),
    ("b", "q", 1),
    ("c", "q", 1),
    ("x", "k", 2),
    ("pk", 0),
    ("s4", "k"),
    ("x", "k", 3),
    ("a", "q", 2),
    ("b", "q", 2),
    ("pk", 1),
    ("pk", 2),
    ("last", "k"),
    ("pk", 3),
    ("pk", 4),
    ("ropek",),
    ("pq", 0),
    ("c", "q", 2),
    ("own", "v"),
    ("x", "q", 1),
    ("s3", "q"),
    ("cross", "v"),
    ("pq", 1),
    ("x", "q", 2),
    ("a", "v", 1),
    ("b", "v", 1),
    ("s4", "q"),
    ("c", "v", 1),
    ("pq", 2),
    ("a", "v", 2),
    ("x", "q", 3),
    ("b", "v", 2),
    ("c", "v", 2),
    ("pq", 3),
    ("x", "v", 1),
    ("last", "q"),
    ("own", "o"),
    ("s3", "v"),
    ("pq", 4),
    ("ropeq",),
)
BETWEEN = (
    (),
    (("cross", "o"), ("a", "o", 1), ),
    (("x", "v", 2), ("s4", "v"), ("x", "v", 3), ("b", "o", 1), ("c", "o", 1), ),
    (),
    (("last", "v"), ("a", "o", 2), ),
    (("b", "o", 2), ),
    (("c", "o", 2), ("x", "o", 1), ),
)
AFTER = (
    ("fin",),
    ("comp", 0),
    ("comp", 1),
    ("s3", "o"),
    ("x", "o", 2),
    ("pair", 0),
    ("s4", "o"),
    ("pair", 1),
    ("comp", 2),
    ("x", "o", 3),
    ("comp", 3),
    ("across", 0),
    ("last", "o"),
    ("comp", 4),
    ("pair", 2),
    ("across", 1),
    ("pair", 4),
    ("pair", 3),
    ("across", 2),
    ("across", 3),
    ("done", 1),
    ("done", 0),
    ("across", 4),
    ("done", 2),
    ("done", 3),
    ("done", 4),
)
SCALE2 = HEAD_DIM**-0.5 * 1.4426950408889634


def wrap(value, size):
    return lax.rem(value + size, size)


class Gather:
    def __init__(self, kind, buf, rows, place, recv, sib_sem, send_sem):
        self.kind, self.buf, self.rows, self.half = kind, buf, rows, rows // 2
        self.x, self.z, self.c, self.head = place
        self.recv, self.sib_sem, self.send_sem = recv, sib_sem, send_sem
        self.zp = self.at(self.x, 1)
        self.zm = self.at(self.x, -1)
        self.xp = self.at(1 - self.x, 0)
        self.sib = (self.x * ZS + self.z) * 2 + 1 - self.c

    def at(self, x, dz):
        return (x * ZS + wrap(self.z + dz, ZS)) * 2 + self.c

    def copy(self, s, part, dev, sem):
        ref = self.buf.at[pl.ds(pl.multiple_of(s * self.rows + part * self.half, 16), self.half)]
        return pltpu.make_async_remote_copy(
            src_ref=ref,
            dst_ref=ref,
            send_sem=self.send_sem.at[self.kind],
            recv_sem=sem,
            device_id=(dev, self.head),
            device_id_type=MESH,
        )

    def sem(self, s, part):
        return self.recv.at[self.kind, lax.div(s, 2), part]

    def send(self, k, other, s, part, *devs):
        for dev in devs:
            self.copy(s, part, dev, self.sem(s, part)).start()
        self.copy(s, part, self.sib, self.sib_sem.at[self.kind, k + 5 * other]).start()

    def relay(self, k, other, dz, part, *devs):
        s = self.at(1 - self.x if other else self.x, dz)
        self.copy(s, part, self.sib, self.sem(s, part)).wait_recv()
        self.send(k, other, s, part, *devs)

    def own(self):
        for part in (0, 1):
            self.send(0, 0, self.at(self.x, 0), part, self.zp, self.zm, self.xp)

    def cross(self):
        self.relay(0, 1, 0, 0, self.zp, self.zm)
        self.relay(0, 1, 0, 1)

    def a(self, k):
        self.relay(k, 0, -k, 0, self.zp)
        self.relay(k, 0, k, 0, self.zm)

    def b(self, k):
        self.relay(k, 0, -k, 1, self.zp, self.xp)
        self.relay(k, 0, k, 1, self.zm, self.xp)

    def c2(self, k):
        self.relay(k, 1, -k, 0, self.zp)
        self.relay(k, 1, k, 0, self.zm)

    def x2(self, k):
        self.relay(k, 1, -k, 1)
        self.relay(k, 1, k, 1)

    def s3(self):
        self.relay(3, 0, -3, 0, self.zp)
        self.relay(3, 0, 3, 1, self.zm, self.xp)
        self.relay(3, 0, -3, 1, self.xp)
        self.relay(3, 0, 3, 0)
        self.relay(3, 1, -3, 0)
        self.relay(3, 1, 3, 0)

    def s4(self):
        self.relay(4, 0, 4, 0, self.xp)
        self.relay(4, 0, 4, 1, self.xp)

    def last(self):
        self.relay(4, 1, 4, 0)
        self.relay(4, 1, 4, 1)

    def sibling(self, k, *others):
        for other in others:
            part = self.buf.at[pl.ds(0, (1 if k in (0, 4) else 2) * self.rows)]
            pltpu.make_async_copy(part, part, self.sib_sem.at[self.kind, k + 5 * other]).wait()

    def drain(self):
        part = self.buf.at[pl.ds(0, 31 * self.rows)]
        pltpu.make_async_copy(part, part, self.send_sem.at[self.kind]).wait()


def rotated(values, cs, sn):
    return values * cs + pltpu.roll(values, HEAD_DIM // 2, 1) * sn


def kernel(
    hidden, gain_hbm, bq_hbm, bk_hbm, bv_hbm, wq_in, wk_in, wv_in, wo_in, table_hbm, out_hbm,
    hid, wkv, wq, kv, wo, kacc, qacc, qs, cs, sn, tmp, att32, att, terms, r1, r2, xs, xr, tot, keep,
    scores0, scores1, high, acc, vecs, out, out_sem, att_rows, gain_in, bq_in, bk_in, bv_in, table, x_terms, x_recv, x_sum, x_wide, x_r1, x_r2, local, recv, sib_sem, send_sem, rsem, r_send,
):
    s = lax.axis_index("seq")
    head = lax.axis_index("head")
    c = lax.rem(s, 2)
    chip = lax.div(s, 2)
    z = lax.rem(chip, ZS)
    x = lax.div(chip, ZS)
    y = lax.rem(head, YS)
    xh = lax.div(head, YS)
    place = (x, z, c, head)
    gather = functools.partial(Gather, place=place, recv=recv, sib_sem=sib_sem, send_sem=send_sem)
    g_kv_w = gather(0, wkv, 256)
    g_q_w = gather(1, wq, 256)
    g_kv = gather(2, kv, ROWS)
    g_o_w = gather(3, wo, 512)
    yp = xh * YS + wrap(y + 1, YS)
    ym = xh * YS + wrap(y - 1, YS)
    xhp = (1 - xh) * YS + y

    mine = pl.ds(pl.multiple_of(s * 256, 256), 256)
    mine_o = pl.ds(pl.multiple_of(s * 512, 512), 512)
    copies = [
        pltpu.make_async_copy(wk_in, wkv.at[mine, pl.ds(0, 128)], local.at[0]),
        pltpu.make_async_copy(wv_in, wkv.at[mine, pl.ds(128, 128)], local.at[1]),
        pltpu.make_async_copy(wq_in, wq.at[mine], local.at[2]),
        pltpu.make_async_copy(hidden, hid, local.at[3]),
        pltpu.make_async_copy(wo_in, wo.at[mine_o], local.at[4]),
        pltpu.make_async_copy(gain_hbm, gain_in, local.at[5]),
        pltpu.make_async_copy(bq_hbm, bq_in, local.at[6]),
        pltpu.make_async_copy(bk_hbm, bk_in, local.at[7]),
        pltpu.make_async_copy(bv_hbm, bv_in, local.at[8]),
        pltpu.make_async_copy(table_hbm, table, local.at[9]),
    ]
    barrier = pltpu.get_barrier_semaphore()
    for dev in (g_q_w.zp, g_q_w.zm, g_q_w.xp, g_q_w.sib):
        pl.semaphore_signal(barrier, inc=1, device_id=(dev, head), device_id_type=MESH)
    for dev in (yp, ym, xhp):
        pl.semaphore_signal(barrier, inc=1, device_id=(s, dev), device_id_type=MESH)
    for copy in copies:
        copy.start()
    copies[0].wait()
    copies[1].wait()
    copies[2].wait()
    pl.semaphore_wait(barrier, 7)
    kinds = {"k": g_kv_w, "q": g_q_w, "v": g_kv, "o": g_o_w}

    def norm(chunk):
        if chunk == 0:
            tables()
            copies[3].wait()

        @pl.loop(3 * chunk, 3 * chunk + 3)
        def _(i):
            rows = pl.ds(pl.multiple_of(i * 16, 16), 16)
            squares = jnp.zeros((16, 1024), F32)
            for j in range(8):
                part = hid[rows, pl.ds(j * 1024, 1024)].astype(F32)
                squares = squares + part * part
            inverse = lax.rsqrt(jnp.sum(squares, axis=-1, keepdims=True) * (1.0 / D) + EPSILON)
            for j in range(8):
                cols = pl.ds(j * 1024, 1024)
                part = hid[rows, cols].astype(F32)
                hid[rows, cols] = (part * inverse * vecs[:, cols]).astype(BF16)

    def tables():
        for copy in copies[5:]:
            copy.wait()
        for i in range(D // HEAD_DIM):
            vecs[:, pl.ds(i * HEAD_DIM, HEAD_DIM)] = gain_in[pl.ds(i, 1), :].astype(F32)
        for i in range(4):
            vecs[:, pl.ds(D + i * HEAD_DIM, HEAD_DIM)] = bq_in[pl.ds(i, 1), :].astype(F32)
        vecs[:, pl.ds(D + 512, HEAD_DIM)] = bk_in[...].astype(F32)
        vecs[:, pl.ds(D + 640, HEAD_DIM)] = bv_in[...].astype(F32)
        cos_row, sin_row = table[0:ROWS, :], table[ROWS : 2 * ROWS, :]
        cos_first = table[pl.ds(2 * ROWS + s, 1), :]
        sin_first = table[pl.ds(2 * ROWS + SEQ + s, 1), :]
        cs[...] = cos_first * cos_row - sin_first * sin_row
        sine = sin_first * cos_row + cos_first * sin_row
        lane = lax.broadcasted_iota(jnp.int32, (ROWS, HEAD_DIM), 1)
        sn[...] = jnp.where(lane < HEAD_DIM // 2, -sine, sine)

    def project(gather, sums, k):
        gather.sibling(k, 0, 1)
        total = None
        for other in (0, 1):
            for dz in (0,) if k == 0 else (4,) if k == 4 else (-k, k):
                place = lax.div(gather.at(1 - x if other else x, dz), 2)
                depth = pl.ds(pl.multiple_of(place * 512, 512), 512)
                term = jnp.dot(hid[:, depth], gather.buf[depth, :], preferred_element_type=F32)
                total = term if total is None else total + term
        sums[...] = total if k == 0 else sums[...] + total

    def store_kv():
        own_kv = pl.ds(pl.multiple_of(s * ROWS, 16), ROWS)
        bk = vecs[:, D + 512 : D + 640]
        bv = vecs[:, D + 640 : D + 768]
        kv[own_kv, 0:128] = rotated(kacc[:, 0:128] + bk, cs[...], sn[...]).astype(BF16)
        kv[own_kv, 128:256] = (kacc[:, 128:256] + bv).astype(BF16)

    def store_q():
        for j in range(4):
            cols = pl.ds(j * HEAD_DIM, HEAD_DIM)
            value = qacc[:, cols] + vecs[:, pl.ds(D + j * HEAD_DIM, HEAD_DIM)]
            qs[pl.ds(j * ROWS, ROWS), :] = rotated(value, cs[...], sn[...]).astype(BF16)

    last_block = lax.div(s, 4)
    score_bufs = (scores0, scores1)

    def set_scores(j, block):
        keys = kv[pl.ds(pl.multiple_of(block * KBLOCK, KBLOCK), KBLOCK), 0:128]
        score_bufs[j % 2][...] = lax.dot_general(
            qs[pl.ds(j * ROWS, ROWS), :], keys, (((1,), (1,)), ((), ())), preferred_element_type=F32
        )

    def attend(block, following, diagonal):
        values = kv[pl.ds(pl.multiple_of(block * KBLOCK, KBLOCK), KBLOCK), 128:256]
        weights = jnp.concatenate([values, jnp.ones((KBLOCK, HEAD_DIM), BF16)], axis=1)
        for j in range(4):
            rows = pl.ds(j * ROWS, ROWS)
            set_scores((j + 1) % 4, block if j < 3 else following)
            scores = score_bufs[j % 2][...]
            if diagonal:
                query_pos = s * ROWS + lax.broadcasted_iota(jnp.int32, (ROWS, KBLOCK), 0)
                key_pos = block * KBLOCK + lax.broadcasted_iota(jnp.int32, (ROWS, KBLOCK), 1)
                scores = jnp.where(query_pos >= key_pos, scores, -jnp.inf)
            new_high = jnp.broadcast_to(jnp.max(scores, axis=-1, keepdims=True), (ROWS, HEAD_DIM))
            if not diagonal:
                old_high = high[rows, :]
                new_high = jnp.maximum(old_high, new_high)
            probs = jnp.exp2((scores - jnp.tile(new_high, (1, KBLOCK // HEAD_DIM))) * SCALE2)
            mixed = jnp.dot(probs.astype(BF16), weights, preferred_element_type=F32)
            if not diagonal:
                fade = jnp.exp2((old_high - new_high) * SCALE2)
                mixed = acc[rows, :] * jnp.tile(fade, (1, 2)) + mixed
            acc[rows, :] = mixed
            high[rows, :] = new_high

    def block_at(i):
        own = (i < 3) | (i == 6)
        column = jnp.where(own, x, 1 - x)
        step = jnp.where(i >= 6, 2, jnp.where(i < 3, jnp.where(i == 2, 1, -i), jnp.where(i == 5, 1, 3 - i)))
        return 4 * column + lax.rem(lax.div(z, 2) + step + 4, 4)

    def arrived(i):
        for k, other in {0: ((0, 0), (1, 0), (2, 0), (3, 0)), 2: ((0, 1), (1, 1)), 3: ((2, 1), (3, 1)), 5: ((4, 0),), 6: ((4, 1),)}.get(i, ()):
            g_kv.sibling(k, other)

    def finish_attention():
        att32[...] = jnp.zeros(att32.shape, F32)
        for j in range(4):
            rows = pl.ds(j * ROWS, ROWS)
            tmp[...] = acc[rows, 0:HEAD_DIM] / acc[rows, HEAD_DIM : 2 * HEAD_DIM]
            att_rows[:, pl.ds(j * HEAD_DIM, HEAD_DIM)] = tmp[...].astype(BF16)
            for h in range(8):
                spot = PADROWS * (h % YS) + OWN * (h // YS)
                att32[pl.ds(spot, OWN), pl.ds(j * HEAD_DIM, HEAD_DIM)] = tmp[pl.ds(h * OWN, OWN), :]
        att[...] = att32[...].astype(BF16)

    y2 = wrap(y + 2, YS)
    y_next = wrap(y + 1, YS)
    y_prev = wrap(y - 1, YS)

    def move(src, dst, kind, g, dev):
        return pltpu.make_async_remote_copy(
            src_ref=src,
            dst_ref=dst,
            send_sem=r_send.at[kind, g],
            recv_sem=rsem.at[kind, g],
            device_id=(s, dev),
            device_id_type=MESH,
        )

    def first(g, kind):
        half = COLS[g] // 2
        cols = pl.ds(BASE[g] + kind * half, half)
        near = r1.at[kind, :, pl.ds(BASE[g] // 2, half)]
        return move(terms.at[y2, :, cols], near, kind, g, ym if kind else yp)

    def second(g, kind):
        cols = pl.ds(BASE[g], COLS[g])
        row = y_prev if kind else y_next
        return move(terms.at[row, :, cols], r2.at[kind, :, cols], 2 + kind, g, ym if kind else yp)

    def third(g):
        cols = pl.ds(BASE[g], COLS[g])
        return move(xs.at[:, cols], xr.at[:, cols], 4, g, xhp)

    def slot_of(g, i):
        ends = g in (0, 4)
        other = lax.div(i, 2 if ends else 4)
        side = 0 if ends else lax.rem(lax.div(i, 2), 2)
        core = lax.rem(i, 2)
        xx = x + other - 2 * x * other
        return (xx * ZS + wrap(z + g - 2 * g * side, ZS)) * 2 + c + core - 2 * c * core

    def compute(g):
        g_o_w.sibling(g, 0, 1)

        @pl.loop(0, COLS[g] // 256)
        def _(i):
            depth = pl.ds(pl.multiple_of(slot_of(g, i) * 512, 512), 512)
            cols = pl.ds(pl.multiple_of(BASE[g] + i * 256, 256), 256)
            term = jnp.dot(att[...], wo[depth, :], preferred_element_type=F32).astype(BF16)
            for k in range(YS):
                terms[k, :, cols] = term[PADROWS * k : PADROWS * k + 2 * OWN]

        first(g, 0).start()
        first(g, 1).start()

    def pair(g):
        for kind in (0, 1):
            first(g, kind).wait_recv()
            row = y_prev if kind else y_next
            half = COLS[g] // 2
            cols = pl.ds(BASE[g] + kind * half, half)
            near = r1[kind, :, pl.ds(BASE[g] // 2, half)].astype(F32)
            terms[row, :, cols] = (terms[row, :, cols].astype(F32) + near).astype(BF16)
            second(g, kind).start()

    def across(g):
        second(g, 0).wait_recv()
        second(g, 1).wait_recv()
        cols = pl.ds(BASE[g], COLS[g])
        part = tot.at[:, pl.ds(0, COLS[g])]
        part[...] = terms[y, :, cols].astype(F32) + r2[0, :, cols].astype(F32) + r2[1, :, cols].astype(F32)
        low, high_rows = part[0:OWN, :], part[OWN : 2 * OWN, :]
        lower = xh == 0
        xs[:, cols] = jnp.where(lower, high_rows, low).astype(BF16)
        keep[:, cols] = jnp.where(lower, low, high_rows)
        third(g).start()

    def done(g):
        third(g).wait_recv()

        @pl.loop(0, COLS[g] // 256)
        def _(i):
            cols = pl.ds(pl.multiple_of(BASE[g] + i * 256, 256), 256)
            there = pl.ds(pl.multiple_of(slot_of(g, i) * 256, 256), 256)
            out[:, there] = (keep[:, cols] + xr[:, cols].astype(F32)).astype(BF16)
            pltpu.make_async_copy(out.at[:, there], out_hbm.at[:, there], out_sem).start()

    def x_cols(g):
        return pl.ds(XBASE[g], COLS[g])

    def x_first(g):
        return move(x_terms.at[1 - xh, :, x_cols(g)], x_recv.at[:, x_cols(g)], 4, g, xhp)

    def x_second(g, kind):
        half = COLS[g] // 2
        near = x_r1.at[kind, :, pl.ds(XBASE[g] // 2, half)]
        return move(x_sum.at[y2, :, pl.ds(XBASE[g] + kind * half, half)], near, kind, g, ym if kind else yp)

    def x_third(g, kind):
        row = y_prev if kind else y_next
        return move(x_sum.at[row, :, x_cols(g)], x_r2.at[kind, :, x_cols(g)], 2 + kind, g, ym if kind else yp)

    def x_compute(g):
        g_o_w.sibling(g, 0, 1)

        @pl.loop(0, COLS[g] // 256)
        def _(i):
            depth = pl.ds(pl.multiple_of(slot_of(g, i) * 512, 512), 512)
            cols = pl.ds(pl.multiple_of(XBASE[g] + i * 256, 256), 256)
            term = jnp.dot(att_rows[...], wo[depth, :], preferred_element_type=F32).astype(BF16)
            for k in range(2):
                x_terms[k, :, cols] = term[ROWS // 2 * k : ROWS // 2 * (k + 1)]

        x_first(g).start()

    def x_pair(g):
        x_first(g).wait_recv()
        wide = x_wide.at[:, pl.ds(0, COLS[g])]
        wide[...] = x_terms[xh, :, x_cols(g)].astype(F32) + x_recv[:, x_cols(g)].astype(F32)
        for k in range(YS):
            x_sum[k, :, x_cols(g)] = wide[pl.ds(OWN * k, OWN), :].astype(BF16)
        x_second(g, 0).start()
        x_second(g, 1).start()

    def x_across(g):
        half = COLS[g] // 2
        for kind in (0, 1):
            x_second(g, kind).wait_recv()
            row = y_prev if kind else y_next
            cols = pl.ds(XBASE[g] + kind * half, half)
            near = x_r1[kind, :, pl.ds(XBASE[g] // 2, half)].astype(F32)
            x_sum[row, :, cols] = (x_sum[row, :, cols].astype(F32) + near).astype(BF16)
            x_third(g, kind).start()

    def x_done(g):
        x_third(g, 0).wait_recv()
        x_third(g, 1).wait_recv()

        @pl.loop(0, COLS[g] // 256)
        def _(i):
            cols = pl.ds(pl.multiple_of(XBASE[g] + i * 256, 256), 256)
            there = pl.ds(pl.multiple_of(slot_of(g, i) * 256, 256), 256)
            value = x_sum[y, :, cols].astype(F32) + x_r2[0, :, cols].astype(F32)
            out[:, there] = (value + x_r2[1, :, cols].astype(F32)).astype(BF16)
            pltpu.make_async_copy(out.at[:, there], out_hbm.at[:, there], out_sem).start()

    x_stages = {"comp": x_compute, "pair": x_pair, "across": x_across, "done": x_done}

    def run(op):
        name, rest = op[0], op[1:]
        if name in ("own", "cross", "s3", "s4", "last"):
            if op == ("own", "o"):
                copies[4].wait()
            getattr(kinds[rest[0]], name)()
        elif name in ("a", "b"):
            getattr(kinds[rest[0]], name)(rest[1])
        elif name in ("c", "x"):
            getattr(kinds[rest[0]], name + "2")(rest[1])
        elif name == "pk":
            project(g_kv_w, kacc, rest[0])
        elif name == "pq":
            project(g_q_w, qacc, rest[0])
        elif name in x_stages and rest[0] in XBASE:
            x_stages[name](rest[0])
        else:
            simple[name](*rest)

    simple = {
        "norm": norm,
        "ropek": store_kv,
        "ropeq": store_q,
        "fin": finish_attention,
        "comp": compute,
        "pair": pair,
        "across": across,
        "done": done,
    }
    for op in BEFORE:
        run(op)
    arrived(0)
    set_scores(0, last_block)
    attend(last_block, block_at(1), True)

    @pl.loop(1, 8)
    def _(i):
        for n, ops in enumerate(BETWEEN):

            @pl.when(i == n + 1)
            def _():
                for op in ops:
                    run(op)
                arrived(n + 1)

        block, following = block_at(i), block_at(jnp.minimum(i + 1, 7))

        @pl.when(block < last_block)
        def _():
            attend(block, following, False)

        @pl.when(block >= last_block)
        def _():
            set_scores(0, following)

    for op in AFTER:
        run(op)

    for g in range(GROUPS):
        one, two, three = (x_second, x_third, x_first) if g in XBASE else (first, second, third)
        for kind in (0, 1):
            one(g, kind).wait_send()
            two(g, kind).wait_send()
        three(g).wait_send()
    for g in (g_kv_w, g_q_w, g_kv, g_o_w):
        g.drain()
    pltpu.make_async_copy(out, out_hbm, out_sem).wait()


def rotary_table():
    half_dim = HEAD_DIM // 2
    freq = ROPE_BASE ** (-2.0 * np.arange(half_dim) / HEAD_DIM)
    rows = np.arange(ROWS)[:, None] * freq
    firsts = ROWS * np.arange(SEQ)[:, None] * freq
    parts = (np.cos(rows), np.sin(rows), np.cos(firsts), np.sin(firsts))
    return np.tile(np.concatenate(parts, axis=0), (1, 2)).astype(np.float32)


def local(hidden, norm_gain, w_query, w_key, w_value, bias_query, bias_key, bias_value, w_out):
    vmem = pl.BlockSpec(memory_space=pltpu.VMEM)
    hbm = pl.BlockSpec(memory_space=pl.ANY)
    dma = pltpu.SemaphoreType.DMA
    return pl.pallas_call(
        kernel,
        name="layer",
        out_shape=jax.ShapeDtypeStruct((OWN, D), BF16),
        in_specs=[hbm] * 10,
        out_specs=hbm,
        scratch_shapes=[
            pltpu.VMEM((ROWS, D), BF16),
            pltpu.VMEM((D, 256), BF16),
            pltpu.VMEM((D, 512), BF16),
            pltpu.VMEM((SEQ * ROWS, 256), BF16),
            pltpu.VMEM((SEQ * 512, 256), BF16),
            pltpu.VMEM((ROWS, 256), F32),
            pltpu.VMEM((ROWS, 512), F32),
            pltpu.VMEM((4 * ROWS, HEAD_DIM), BF16),
            pltpu.VMEM((ROWS, HEAD_DIM), F32),
            pltpu.VMEM((ROWS, HEAD_DIM), F32),
            pltpu.VMEM((ROWS, HEAD_DIM), F32),
            pltpu.VMEM((YS * PADROWS, 512), F32),
            pltpu.VMEM((YS * PADROWS, 512), BF16),
            pltpu.VMEM((YS, 2 * OWN, D), BF16),
            pltpu.VMEM((2, 2 * OWN, D // 2), BF16),
            pltpu.VMEM((2, 2 * OWN, D), BF16),
            pltpu.VMEM((OWN, D), BF16),
            pltpu.VMEM((OWN, D), BF16),
            pltpu.VMEM((2 * OWN, 2048), F32),
            pltpu.VMEM((OWN, D), F32),
            pltpu.VMEM((ROWS, KBLOCK), F32),
            pltpu.VMEM((ROWS, KBLOCK), F32),
            pltpu.VMEM((4 * ROWS, HEAD_DIM), F32),
            pltpu.VMEM((4 * ROWS, 2 * HEAD_DIM), F32),
            pltpu.VMEM((1, D + 768), F32),
            pltpu.VMEM((OWN, D), BF16),
            dma,
            pltpu.VMEM((ROWS, 512), BF16),
            pltpu.VMEM((D // HEAD_DIM, HEAD_DIM), BF16),
            pltpu.VMEM((4, HEAD_DIM), BF16),
            pltpu.VMEM((1, HEAD_DIM), BF16),
            pltpu.VMEM((1, HEAD_DIM), BF16),
            pltpu.VMEM((2 * ROWS + 2 * SEQ, HEAD_DIM), F32),
            pltpu.VMEM((2, ROWS // 2, XCOLS), BF16),
            pltpu.VMEM((ROWS // 2, XCOLS), BF16),
            pltpu.VMEM((YS, OWN, XCOLS), BF16),
            pltpu.VMEM((ROWS // 2, 2048), F32),
            pltpu.VMEM((2, OWN, XCOLS // 2), BF16),
            pltpu.VMEM((2, OWN, XCOLS), BF16),
            dma((10,)),
            dma((4, 16, 2)),
            dma((4,10)),
            dma((4,)),
            dma((5, GROUPS)),
            dma((5, GROUPS)),
        ],
        compiler_params=pltpu.CompilerParams(
            collective_id=0, has_side_effects=True, vmem_limit_bytes=66 * 1000 * 1000
        ),
    )(
        hidden, norm_gain.reshape(-1, HEAD_DIM), bias_query.reshape(-1, HEAD_DIM),
        bias_key.reshape(-1, HEAD_DIM), bias_value.reshape(-1, HEAD_DIM),
        w_query, w_key, w_value, w_out, jnp.asarray(rotary_table()),
    )


def solution(mesh):
    in_specs = (
        P("seq", None),
        P(),
        P("seq", "head"),
        P("seq", "head"),
        P("seq", "head"),
        P("head"),
        P("head"),
        P("head"),
        P("head", "seq"),
    )
    out_specs = P(("seq", "head"), None)
    return jax.shard_map(local, mesh=mesh, in_specs=in_specs, out_specs=out_specs, check_vma=False)
```

```python
import functools

import jax
import jax.numpy as jnp
import numpy as np
from jax import lax
from jax.experimental import pallas as pl
from jax.experimental.pallas import tpu as pltpu
from jax.sharding import PartitionSpec as P

HEAD_DIM = 128
ROPE_BASE = 1000000.0
EPSILON = 1e-06
BF16 = jnp.bfloat16
F32 = jnp.float32
MESH = pl.DeviceIdType.MESH
ZS = 8
YS = 4
SEQ = 32
ROWS = 288
D = 8192
OWN = 36
GROUPS = 8
DISTANCE = (0, 1, 1, 2, 2, 3, 3, 4)
COLS = (1024,) * GROUPS
BASE = tuple(1024 * g for g in range(GROUPS))
KBLOCK = 1152
PADROWS = 80
XBASE = {5: 0, 6: 1024}
XCOLS = 2048
BEFORE = (
    ("own", "k"),
    ("norm", 0),
    ("own", "q"),
    ("cross", "k"),
    ("norm", 1),
    ("a", "k", 1),
    ("b", "k", 1),
    ("c", "k", 1),
    ("norm", 2),
    ("a", "k", 2),
    ("norm", 3),
    ("norm", 4),
    ("b", "k", 2),
    ("c", "k", 2),
    ("x", "k", 1),
    ("cross", "q"),
    ("norm", 5),
    ("a", "q", 1),
    ("s3", "k"),
    ("b", "q", 1),
    ("c", "q", 1),
    ("x", "k", 2),
    ("pk", 0),
    ("s4", "k"),
    ("x", "k", 3),
    ("a", "q", 2),
    ("b", "q", 2),
    ("pk", 1),
    ("pk", 2),
    ("last", "k"),
    ("pk", 3),
    ("pk", 4),
    ("ropek",),
    ("pq", 0),
    ("c", "q", 2),
    ("own", "v"),
    ("x", "q", 1),
    ("s3", "q"),
    ("cross", "v"),
    ("pq", 1),
    ("x", "q", 2),
    ("a", "v", 1),
    ("b", "v", 1),
    ("s4", "q"),
    ("c", "v", 1),
    ("pq", 2),
    ("a", "v", 2),
    ("x", "q", 3),
    ("b", "v", 2),
    ("c", "v", 2),
    ("pq", 3),
    ("x", "v", 1),
    ("last", "q"),
    ("own", "o"),
    ("s3", "v"),
    ("pq", 4),
    ("ropeq",),
)
BETWEEN = (
    (),
    (("cross", "o"), ("a", "o", 1), ),
    (("x", "v", 2), ("s4", "v"), ("x", "v", 3), ("b", "o", 1), ("c", "o", 1), ),
    (),
    (("last", "v"), ("a", "o", 2), ),
    (("b", "o", 2), ),
    (("c", "o", 2), ("x", "o", 1), ),
)
AFTER = (
    ("fin",),
    ("comp", 0),
    ("comp", 1),
    ("comp", 2),
    ("s3", "o"),
    ("x", "o", 2),
    ("pair", 0),
    ("s4", "o"),
    ("pair", 1),
    ("pair", 2),
    ("comp", 3),
    ("comp", 4),
    ("x", "o", 3),
    ("comp", 5),
    ("comp", 6),
    ("across", 0),
    ("last", "o"),
    ("comp", 7),
    ("pair", 3),
    ("pair", 4),
    ("across", 1),
    ("across", 2),
    ("pair", 7),
    ("pair", 5),
    ("pair", 6),
    ("across", 3),
    ("across", 4),
    ("across", 5),
    ("across", 6),
    ("done", 1),
    ("done", 2),
    ("done", 0),
    ("across", 7),
    ("done", 3),
    ("done", 4),
    ("done", 5),
    ("done", 6),
    ("done", 7),
)
SCALE2 = HEAD_DIM**-0.5 * 1.4426950408889634


def wrap(value, size):
    return lax.rem(value + size, size)


class Gather:
    def __init__(self, kind, buf, rows, place, recv, sib_sem, send_sem):
        self.kind, self.buf, self.rows, self.half = kind, buf, rows, rows // 2
        self.x, self.z, self.c, self.head = place
        self.recv, self.sib_sem, self.send_sem = recv, sib_sem, send_sem
        self.zp = self.at(self.x, 1)
        self.zm = self.at(self.x, -1)
        self.xp = self.at(1 - self.x, 0)
        self.sib = (self.x * ZS + self.z) * 2 + 1 - self.c

    def at(self, x, dz):
        return (x * ZS + wrap(self.z + dz, ZS)) * 2 + self.c

    def copy(self, s, part, dev, sem):
        ref = self.buf.at[pl.ds(pl.multiple_of(s * self.rows + part * self.half, 16), self.half)]
        return pltpu.make_async_remote_copy(
            src_ref=ref,
            dst_ref=ref,
            send_sem=self.send_sem.at[self.kind],
            recv_sem=sem,
            device_id=(dev, self.head),
            device_id_type=MESH,
        )

    def sem(self, s, part):
        return self.recv.at[self.kind, lax.div(s, 2), part]

    def send(self, k, other, s, part, *devs):
        for dev in devs:
            self.copy(s, part, dev, self.sem(s, part)).start()
        self.copy(s, part, self.sib, self.sib_sem.at[self.kind, k + 5 * other]).start()

    def relay(self, k, other, dz, part, *devs):
        s = self.at(1 - self.x if other else self.x, dz)
        self.copy(s, part, self.sib, self.sem(s, part)).wait_recv()
        self.send(k, other, s, part, *devs)

    def own(self):
        for part in (0, 1):
            self.send(0, 0, self.at(self.x, 0), part, self.zp, self.zm, self.xp)

    def cross(self):
        self.relay(0, 1, 0, 0, self.zp, self.zm)
        self.relay(0, 1, 0, 1)

    def a(self, k):
        self.relay(k, 0, -k, 0, self.zp)
        self.relay(k, 0, k, 0, self.zm)

    def b(self, k):
        self.relay(k, 0, -k, 1, self.zp, self.xp)
        self.relay(k, 0, k, 1, self.zm, self.xp)

    def c2(self, k):
        self.relay(k, 1, -k, 0, self.zp)
        self.relay(k, 1, k, 0, self.zm)

    def x2(self, k):
        self.relay(k, 1, -k, 1)
        self.relay(k, 1, k, 1)

    def s3(self):
        self.relay(3, 0, -3, 0, self.zp)
        self.relay(3, 0, 3, 1, self.zm, self.xp)
        self.relay(3, 0, -3, 1, self.xp)
        self.relay(3, 0, 3, 0)
        self.relay(3, 1, -3, 0)
        self.relay(3, 1, 3, 0)

    def s4(self):
        self.relay(4, 0, 4, 0, self.xp)
        self.relay(4, 0, 4, 1, self.xp)

    def last(self):
        self.relay(4, 1, 4, 0)
        self.relay(4, 1, 4, 1)

    def sibling(self, k, *others):
        for other in others:
            part = self.buf.at[pl.ds(0, (1 if k in (0, 4) else 2) * self.rows)]
            pltpu.make_async_copy(part, part, self.sib_sem.at[self.kind, k + 5 * other]).wait()

    def drain(self):
        part = self.buf.at[pl.ds(0, 31 * self.rows)]
        pltpu.make_async_copy(part, part, self.send_sem.at[self.kind]).wait()


def rotated(values, cs, sn):
    return values * cs + pltpu.roll(values, HEAD_DIM // 2, 1) * sn


def kernel(
    hidden, gain_hbm, bq_hbm, bk_hbm, bv_hbm, wq_in, wk_in, wv_in, wo_in, table_hbm, out_hbm,
    hid, wkv, wq, kv, wo, kacc, qacc, qs, cs, sn, tmp, att32, att, terms, r1, r2, xs, xr, tot, keep,
    scores0, scores1, high, acc, vecs, out, out_sem, att_rows, gain_in, bq_in, bk_in, bv_in, table, x_terms, x_recv, x_sum, x_wide, x_r1, x_r2, local, recv, sib_sem, send_sem, rsem, r_send,
):
    s = lax.axis_index("seq")
    head = lax.axis_index("head")
    c = lax.rem(s, 2)
    chip = lax.div(s, 2)
    z = lax.rem(chip, ZS)
    x = lax.div(chip, ZS)
    y = lax.rem(head, YS)
    xh = lax.div(head, YS)
    place = (x, z, c, head)
    gather = functools.partial(Gather, place=place, recv=recv, sib_sem=sib_sem, send_sem=send_sem)
    g_kv_w = gather(0, wkv, 256)
    g_q_w = gather(1, wq, 256)
    g_kv = gather(2, kv, ROWS)
    g_o_w = gather(3, wo, 512)
    yp = xh * YS + wrap(y + 1, YS)
    ym = xh * YS + wrap(y - 1, YS)
    xhp = (1 - xh) * YS + y

    mine = pl.ds(pl.multiple_of(s * 256, 256), 256)
    mine_o = pl.ds(pl.multiple_of(s * 512, 512), 512)
    copies = [
        pltpu.make_async_copy(wk_in, wkv.at[mine, pl.ds(0, 128)], local.at[0]),
        pltpu.make_async_copy(wv_in, wkv.at[mine, pl.ds(128, 128)], local.at[1]),
        pltpu.make_async_copy(wq_in, wq.at[mine], local.at[2]),
        pltpu.make_async_copy(hidden, hid, local.at[3]),
        pltpu.make_async_copy(wo_in, wo.at[mine_o], local.at[4]),
        pltpu.make_async_copy(gain_hbm, gain_in, local.at[5]),
        pltpu.make_async_copy(bq_hbm, bq_in, local.at[6]),
        pltpu.make_async_copy(bk_hbm, bk_in, local.at[7]),
        pltpu.make_async_copy(bv_hbm, bv_in, local.at[8]),
        pltpu.make_async_copy(table_hbm, table, local.at[9]),
    ]
    barrier = pltpu.get_barrier_semaphore()
    for dev in (g_q_w.zp, g_q_w.zm, g_q_w.xp, g_q_w.sib):
        pl.semaphore_signal(barrier, inc=1, device_id=(dev, head), device_id_type=MESH)
    for dev in (yp, ym, xhp):
        pl.semaphore_signal(barrier, inc=1, device_id=(s, dev), device_id_type=MESH)
    for copy in copies:
        copy.start()
    copies[0].wait()
    copies[1].wait()
    copies[2].wait()
    pl.semaphore_wait(barrier, 7)
    kinds = {"k": g_kv_w, "q": g_q_w, "v": g_kv, "o": g_o_w}

    def norm(chunk):
        if chunk == 0:
            tables()
            copies[3].wait()

        @pl.loop(3 * chunk, 3 * chunk + 3)
        def _(i):
            rows = pl.ds(pl.multiple_of(i * 16, 16), 16)
            squares = jnp.zeros((16, 1024), F32)
            for j in range(8):
                part = hid[rows, pl.ds(j * 1024, 1024)].astype(F32)
                squares = squares + part * part
            inverse = lax.rsqrt(jnp.sum(squares, axis=-1, keepdims=True) * (1.0 / D) + EPSILON)
            for j in range(8):
                cols = pl.ds(j * 1024, 1024)
                part = hid[rows, cols].astype(F32)
                hid[rows, cols] = (part * inverse * vecs[:, cols]).astype(BF16)

    def tables():
        for copy in copies[5:]:
            copy.wait()
        for i in range(D // HEAD_DIM):
            vecs[:, pl.ds(i * HEAD_DIM, HEAD_DIM)] = gain_in[pl.ds(i, 1), :].astype(F32)
        for i in range(4):
            vecs[:, pl.ds(D + i * HEAD_DIM, HEAD_DIM)] = bq_in[pl.ds(i, 1), :].astype(F32)
        vecs[:, pl.ds(D + 512, HEAD_DIM)] = bk_in[...].astype(F32)
        vecs[:, pl.ds(D + 640, HEAD_DIM)] = bv_in[...].astype(F32)
        cos_row, sin_row = table[0:ROWS, :], table[ROWS : 2 * ROWS, :]
        cos_first = table[pl.ds(2 * ROWS + s, 1), :]
        sin_first = table[pl.ds(2 * ROWS + SEQ + s, 1), :]
        cs[...] = cos_first * cos_row - sin_first * sin_row
        sine = sin_first * cos_row + cos_first * sin_row
        lane = lax.broadcasted_iota(jnp.int32, (ROWS, HEAD_DIM), 1)
        sn[...] = jnp.where(lane < HEAD_DIM // 2, -sine, sine)

    def project(gather, sums, k):
        gather.sibling(k, 0, 1)
        total = None
        for other in (0, 1):
            for dz in (0,) if k == 0 else (4,) if k == 4 else (-k, k):
                place = lax.div(gather.at(1 - x if other else x, dz), 2)
                depth = pl.ds(pl.multiple_of(place * 512, 512), 512)
                term = jnp.dot(hid[:, depth], gather.buf[depth, :], preferred_element_type=F32)
                total = term if total is None else total + term
        sums[...] = total if k == 0 else sums[...] + total

    def store_kv():
        own_kv = pl.ds(pl.multiple_of(s * ROWS, 16), ROWS)
        bk = vecs[:, D + 512 : D + 640]
        bv = vecs[:, D + 640 : D + 768]
        kv[own_kv, 0:128] = rotated(kacc[:, 0:128] + bk, cs[...], sn[...]).astype(BF16)
        kv[own_kv, 128:256] = (kacc[:, 128:256] + bv).astype(BF16)

    def store_q():
        for j in range(4):
            cols = pl.ds(j * HEAD_DIM, HEAD_DIM)
            value = qacc[:, cols] + vecs[:, pl.ds(D + j * HEAD_DIM, HEAD_DIM)]
            qs[pl.ds(j * ROWS, ROWS), :] = rotated(value, cs[...], sn[...]).astype(BF16)

    last_block = lax.div(s, 4)
    score_bufs = (scores0, scores1)

    def set_scores(j, block):
        keys = kv[pl.ds(pl.multiple_of(block * KBLOCK, KBLOCK), KBLOCK), 0:128]
        score_bufs[j % 2][...] = lax.dot_general(
            qs[pl.ds(j * ROWS, ROWS), :], keys, (((1,), (1,)), ((), ())), preferred_element_type=F32
        )

    def attend(block, following, diagonal):
        values = kv[pl.ds(pl.multiple_of(block * KBLOCK, KBLOCK), KBLOCK), 128:256]
        for j in range(4):
            rows = pl.ds(j * ROWS, ROWS)
            set_scores((j + 1) % 4, block if j < 3 else following)
            scores = score_bufs[j % 2][...]
            if diagonal:
                query_pos = s * ROWS + lax.broadcasted_iota(jnp.int32, (ROWS, KBLOCK), 0)
                key_pos = block * KBLOCK + lax.broadcasted_iota(jnp.int32, (ROWS, KBLOCK), 1)
                scores = jnp.where(query_pos >= key_pos, scores, -jnp.inf)
            new_high = jnp.broadcast_to(jnp.max(scores, axis=-1, keepdims=True), (ROWS, HEAD_DIM))
            if not diagonal:
                old_high = high[rows, :]
                new_high = jnp.maximum(old_high, new_high)
            probs = jnp.exp2((scores - jnp.tile(new_high, (1, KBLOCK // HEAD_DIM))) * SCALE2)
            part = probs[:, 0:HEAD_DIM]
            for n in range(1, KBLOCK // HEAD_DIM):
                part = part + probs[:, n * HEAD_DIM : (n + 1) * HEAD_DIM]
            mixed = jnp.dot(probs.astype(BF16), values, preferred_element_type=F32)
            if not diagonal:
                fade = jnp.exp2((old_high - new_high) * SCALE2)
                mixed = acc[rows, 0:HEAD_DIM] * fade + mixed
                part = acc[rows, HEAD_DIM : 2 * HEAD_DIM] * fade + part
            acc[rows, 0:HEAD_DIM] = mixed
            acc[rows, HEAD_DIM : 2 * HEAD_DIM] = part
            high[rows, :] = new_high

    def block_at(i):
        own = (i < 3) | (i == 6)
        column = jnp.where(own, x, 1 - x)
        step = jnp.where(i >= 6, 2, jnp.where(i < 3, jnp.where(i == 2, 1, -i), jnp.where(i == 5, 1, 3 - i)))
        return 4 * column + lax.rem(lax.div(z, 2) + step + 4, 4)

    def arrived(i):
        for k, other in {0: ((0, 0), (1, 0), (2, 0), (3, 0)), 2: ((0, 1), (1, 1)), 3: ((2, 1), (3, 1)), 5: ((4, 0),), 6: ((4, 1),)}.get(i, ()):
            g_kv.sibling(k, other)

    def finish_attention():
        att32[...] = jnp.zeros(att32.shape, F32)
        for j in range(4):
            rows = pl.ds(j * ROWS, ROWS)
            tmp[...] = acc[rows, 0:HEAD_DIM] / jnp.sum(
                acc[rows, HEAD_DIM : 2 * HEAD_DIM], axis=-1, keepdims=True
            )
            att_rows[:, pl.ds(j * HEAD_DIM, HEAD_DIM)] = tmp[...].astype(BF16)
            for h in range(8):
                spot = PADROWS * (h % YS) + OWN * (h // YS)
                att32[pl.ds(spot, OWN), pl.ds(j * HEAD_DIM, HEAD_DIM)] = tmp[pl.ds(h * OWN, OWN), :]
        att[...] = att32[...].astype(BF16)

    y2 = wrap(y + 2, YS)
    y_next = wrap(y + 1, YS)
    y_prev = wrap(y - 1, YS)

    def move(src, dst, kind, g, dev):
        return pltpu.make_async_remote_copy(
            src_ref=src,
            dst_ref=dst,
            send_sem=r_send.at[kind, g],
            recv_sem=rsem.at[kind, g],
            device_id=(s, dev),
            device_id_type=MESH,
        )

    def first(g, kind):
        half = COLS[g] // 2
        cols = pl.ds(BASE[g] + kind * half, half)
        near = r1.at[kind, :, pl.ds(BASE[g] // 2, half)]
        return move(terms.at[y2, :, cols], near, kind, g, ym if kind else yp)

    def second(g, kind):
        cols = pl.ds(BASE[g], COLS[g])
        row = y_prev if kind else y_next
        return move(terms.at[row, :, cols], r2.at[kind, :, cols], 2 + kind, g, ym if kind else yp)

    def third(g):
        cols = pl.ds(BASE[g], COLS[g])
        return move(xs.at[:, cols], xr.at[:, cols], 4, g, xhp)

    def slot_of(g, i):
        k = DISTANCE[g]
        ends = k in (0, 4)
        other = lax.div(i, 2) if ends else 1 - g % 2
        side = 0 if ends else lax.div(i, 2)
        core = lax.rem(i, 2)
        xx = x + other - 2 * x * other
        return (xx * ZS + wrap(z + k - 2 * k * side, ZS)) * 2 + c + core - 2 * c * core

    def shards_in(g):
        k = DISTANCE[g]
        g_o_w.sibling(k, *((0, 1) if k in (0, 4) else (1 - g % 2,)))

    def compute(g):
        shards_in(g)

        @pl.loop(0, COLS[g] // 256)
        def _(i):
            depth = pl.ds(pl.multiple_of(slot_of(g, i) * 512, 512), 512)
            cols = pl.ds(pl.multiple_of(BASE[g] + i * 256, 256), 256)
            term = jnp.dot(att[...], wo[depth, :], preferred_element_type=F32).astype(BF16)
            for k in range(YS):
                terms[k, :, cols] = term[PADROWS * k : PADROWS * k + 2 * OWN]

        first(g, 0).start()
        first(g, 1).start()

    def pair(g):
        for kind in (0, 1):
            first(g, kind).wait_recv()
            row = y_prev if kind else y_next
            half = COLS[g] // 2
            cols = pl.ds(BASE[g] + kind * half, half)
            near = r1[kind, :, pl.ds(BASE[g] // 2, half)].astype(F32)
            terms[row, :, cols] = (terms[row, :, cols].astype(F32) + near).astype(BF16)
            second(g, kind).start()

    def across(g):
        second(g, 0).wait_recv()
        second(g, 1).wait_recv()
        cols = pl.ds(BASE[g], COLS[g])
        part = tot.at[:, pl.ds(0, COLS[g])]
        part[...] = terms[y, :, cols].astype(F32) + r2[0, :, cols].astype(F32) + r2[1, :, cols].astype(F32)
        low, high_rows = part[0:OWN, :], part[OWN : 2 * OWN, :]
        lower = xh == 0
        xs[:, cols] = jnp.where(lower, high_rows, low).astype(BF16)
        keep[:, cols] = jnp.where(lower, low, high_rows)
        third(g).start()

    def done(g):
        third(g).wait_recv()

        @pl.loop(0, COLS[g] // 256)
        def _(i):
            cols = pl.ds(pl.multiple_of(BASE[g] + i * 256, 256), 256)
            there = pl.ds(pl.multiple_of(slot_of(g, i) * 256, 256), 256)
            out[:, there] = (keep[:, cols] + xr[:, cols].astype(F32)).astype(BF16)
            pltpu.make_async_copy(out.at[:, there], out_hbm.at[:, there], out_sem).start()

    def x_cols(g):
        return pl.ds(XBASE[g], COLS[g])

    def x_first(g):
        return move(x_terms.at[1 - xh, :, x_cols(g)], x_recv.at[:, x_cols(g)], 4, g, xhp)

    def x_second(g, kind):
        half = COLS[g] // 2
        near = x_r1.at[kind, :, pl.ds(XBASE[g] // 2, half)]
        return move(x_sum.at[y2, :, pl.ds(XBASE[g] + kind * half, half)], near, kind, g, ym if kind else yp)

    def x_third(g, kind):
        row = y_prev if kind else y_next
        return move(x_sum.at[row, :, x_cols(g)], x_r2.at[kind, :, x_cols(g)], 2 + kind, g, ym if kind else yp)

    def x_compute(g):
        shards_in(g)

        @pl.loop(0, COLS[g] // 256)
        def _(i):
            depth = pl.ds(pl.multiple_of(slot_of(g, i) * 512, 512), 512)
            cols = pl.ds(pl.multiple_of(XBASE[g] + i * 256, 256), 256)
            term = jnp.dot(att_rows[...], wo[depth, :], preferred_element_type=F32).astype(BF16)
            for k in range(2):
                x_terms[k, :, cols] = term[ROWS // 2 * k : ROWS // 2 * (k + 1)]

        x_first(g).start()

    def x_pair(g):
        x_first(g).wait_recv()
        wide = x_wide.at[:, pl.ds(0, COLS[g])]
        wide[...] = x_terms[xh, :, x_cols(g)].astype(F32) + x_recv[:, x_cols(g)].astype(F32)
        for k in range(YS):
            x_sum[k, :, x_cols(g)] = wide[pl.ds(OWN * k, OWN), :].astype(BF16)
        x_second(g, 0).start()
        x_second(g, 1).start()

    def x_across(g):
        half = COLS[g] // 2
        for kind in (0, 1):
            x_second(g, kind).wait_recv()
            row = y_prev if kind else y_next
            cols = pl.ds(XBASE[g] + kind * half, half)
            near = x_r1[kind, :, pl.ds(XBASE[g] // 2, half)].astype(F32)
            x_sum[row, :, cols] = (x_sum[row, :, cols].astype(F32) + near).astype(BF16)
            x_third(g, kind).start()

    def x_done(g):
        x_third(g, 0).wait_recv()
        x_third(g, 1).wait_recv()

        @pl.loop(0, COLS[g] // 256)
        def _(i):
            cols = pl.ds(pl.multiple_of(XBASE[g] + i * 256, 256), 256)
            there = pl.ds(pl.multiple_of(slot_of(g, i) * 256, 256), 256)
            value = x_sum[y, :, cols].astype(F32) + x_r2[0, :, cols].astype(F32)
            out[:, there] = (value + x_r2[1, :, cols].astype(F32)).astype(BF16)
            pltpu.make_async_copy(out.at[:, there], out_hbm.at[:, there], out_sem).start()

    x_stages = {"comp": x_compute, "pair": x_pair, "across": x_across, "done": x_done}

    def run(op):
        name, rest = op[0], op[1:]
        if name in ("own", "cross", "s3", "s4", "last"):
            if op == ("own", "o"):
                copies[4].wait()
            getattr(kinds[rest[0]], name)()
        elif name in ("a", "b"):
            getattr(kinds[rest[0]], name)(rest[1])
        elif name in ("c", "x"):
            getattr(kinds[rest[0]], name + "2")(rest[1])
        elif name == "pk":
            project(g_kv_w, kacc, rest[0])
        elif name == "pq":
            project(g_q_w, qacc, rest[0])
        elif name in x_stages and rest[0] in XBASE:
            x_stages[name](rest[0])
        else:
            simple[name](*rest)

    simple = {
        "norm": norm,
        "ropek": store_kv,
        "ropeq": store_q,
        "fin": finish_attention,
        "comp": compute,
        "pair": pair,
        "across": across,
        "done": done,
    }
    for op in BEFORE:
        run(op)
    arrived(0)
    set_scores(0, last_block)
    attend(last_block, block_at(1), True)

    @pl.loop(1, 8)
    def _(i):
        for n, ops in enumerate(BETWEEN):

            @pl.when(i == n + 1)
            def _():
                for op in ops:
                    run(op)
                arrived(n + 1)

        block, following = block_at(i), block_at(jnp.minimum(i + 1, 7))

        @pl.when(block < last_block)
        def _():
            attend(block, following, False)

        @pl.when(block >= last_block)
        def _():
            set_scores(0, following)

    for op in AFTER:
        run(op)

    for g in range(GROUPS):
        one, two, three = (x_second, x_third, x_first) if g in XBASE else (first, second, third)
        for kind in (0, 1):
            one(g, kind).wait_send()
            two(g, kind).wait_send()
        three(g).wait_send()
    for g in (g_kv_w, g_q_w, g_kv, g_o_w):
        g.drain()
    pltpu.make_async_copy(out, out_hbm, out_sem).wait()


def rotary_table():
    half_dim = HEAD_DIM // 2
    freq = ROPE_BASE ** (-2.0 * np.arange(half_dim) / HEAD_DIM)
    rows = np.arange(ROWS)[:, None] * freq
    firsts = ROWS * np.arange(SEQ)[:, None] * freq
    parts = (np.cos(rows), np.sin(rows), np.cos(firsts), np.sin(firsts))
    return np.tile(np.concatenate(parts, axis=0), (1, 2)).astype(np.float32)


def local(hidden, norm_gain, w_query, w_key, w_value, bias_query, bias_key, bias_value, w_out):
    vmem = pl.BlockSpec(memory_space=pltpu.VMEM)
    hbm = pl.BlockSpec(memory_space=pl.ANY)
    dma = pltpu.SemaphoreType.DMA
    return pl.pallas_call(
        kernel,
        name="layer",
        out_shape=jax.ShapeDtypeStruct((OWN, D), BF16),
        in_specs=[hbm] * 10,
        out_specs=hbm,
        scratch_shapes=[
            pltpu.VMEM((ROWS, D), BF16),
            pltpu.VMEM((D, 256), BF16),
            pltpu.VMEM((D, 512), BF16),
            pltpu.VMEM((SEQ * ROWS, 256), BF16),
            pltpu.VMEM((SEQ * 512, 256), BF16),
            pltpu.VMEM((ROWS, 256), F32),
            pltpu.VMEM((ROWS, 512), F32),
            pltpu.VMEM((4 * ROWS, HEAD_DIM), BF16),
            pltpu.VMEM((ROWS, HEAD_DIM), F32),
            pltpu.VMEM((ROWS, HEAD_DIM), F32),
            pltpu.VMEM((ROWS, HEAD_DIM), F32),
            pltpu.VMEM((YS * PADROWS, 512), F32),
            pltpu.VMEM((YS * PADROWS, 512), BF16),
            pltpu.VMEM((YS, 2 * OWN, D), BF16),
            pltpu.VMEM((2, 2 * OWN, D // 2), BF16),
            pltpu.VMEM((2, 2 * OWN, D), BF16),
            pltpu.VMEM((OWN, D), BF16),
            pltpu.VMEM((OWN, D), BF16),
            pltpu.VMEM((2 * OWN, 1024), F32),
            pltpu.VMEM((OWN, D), F32),
            pltpu.VMEM((ROWS, KBLOCK), F32),
            pltpu.VMEM((ROWS, KBLOCK), F32),
            pltpu.VMEM((4 * ROWS, HEAD_DIM), F32),
            pltpu.VMEM((4 * ROWS, 2 * HEAD_DIM), F32),
            pltpu.VMEM((1, D + 768), F32),
            pltpu.VMEM((OWN, D), BF16),
            dma,
            pltpu.VMEM((ROWS, 512), BF16),
            pltpu.VMEM((D // HEAD_DIM, HEAD_DIM), BF16),
            pltpu.VMEM((4, HEAD_DIM), BF16),
            pltpu.VMEM((1, HEAD_DIM), BF16),
            pltpu.VMEM((1, HEAD_DIM), BF16),
            pltpu.VMEM((2 * ROWS + 2 * SEQ, HEAD_DIM), F32),
            pltpu.VMEM((2, ROWS // 2, XCOLS), BF16),
            pltpu.VMEM((ROWS // 2, XCOLS), BF16),
            pltpu.VMEM((YS, OWN, XCOLS), BF16),
            pltpu.VMEM((ROWS // 2, 1024), F32),
            pltpu.VMEM((2, OWN, XCOLS // 2), BF16),
            pltpu.VMEM((2, OWN, XCOLS), BF16),
            dma((10,)),
            dma((4, 16, 2)),
            dma((4,10)),
            dma((4,)),
            dma((5, GROUPS)),
            dma((5, GROUPS)),
        ],
        compiler_params=pltpu.CompilerParams(
            collective_id=0, has_side_effects=True, vmem_limit_bytes=66 * 1000 * 1000
        ),
    )(
        hidden, norm_gain.reshape(-1, HEAD_DIM), bias_query.reshape(-1, HEAD_DIM),
        bias_key.reshape(-1, HEAD_DIM), bias_value.reshape(-1, HEAD_DIM),
        w_query, w_key, w_value, w_out, jnp.asarray(rotary_table()),
    )


def solution(mesh):
    in_specs = (
        P("seq", None),
        P(),
        P("seq", "head"),
        P("seq", "head"),
        P("seq", "head"),
        P("head"),
        P("head"),
        P("head"),
        P("head", "seq"),
    )
    out_specs = P(("seq", "head"), None)
    return jax.shard_map(local, mesh=mesh, in_specs=in_specs, out_specs=out_specs, check_vma=False)
```

```python
import functools

import jax
import jax.numpy as jnp
import numpy as np
from jax import lax
from jax.experimental import pallas as pl
from jax.experimental.pallas import tpu as pltpu
from jax.sharding import PartitionSpec as P

HEAD_DIM = 128
ROPE_BASE = 1000000.0
EPSILON = 1e-06
BF16 = jnp.bfloat16
F32 = jnp.float32
MESH = pl.DeviceIdType.MESH
ZS = 8
YS = 4
SEQ = 32
ROWS = 288
D = 8192
OWN = 36
GROUPS = 8
DISTANCE = (0, 1, 1, 2, 2, 3, 3, 4)
COLS = (1024,) * GROUPS
BASE = tuple(1024 * g for g in range(GROUPS))
KBLOCK = 1152
PADROWS = 80
XBASE = {1: 0, 6: 1024}
XCOLS = 2048
BEFORE = (
    ("own", "k"),
    ("own", "q"),
    ("cross", "k"),
    ("norm", 0),
    ("norm", 1),
    ("norm", 2),
    ("a", "k", 1),
    ("b", "k", 1),
    ("c", "k", 1),
    ("norm", 3),
    ("a", "k", 2),
    ("b", "k", 2),
    ("c", "k", 2),
    ("x", "k", 1),
    ("cross", "q"),
    ("s3", "k"),
    ("a", "q", 1),
    ("x", "k", 2),
    ("norm", 4),
    ("norm", 5),
    ("b", "q", 1),
    ("pk", 0),
    ("s4", "k"),
    ("c", "q", 1),
    ("a", "q", 2),
    ("x", "k", 3),
    ("pk", 1),
    ("b", "q", 2),
    ("pq", 0),
    ("last", "k"),
    ("c", "q", 2),
    ("pk", 2),
    ("pk", 3),
    ("pk", 4),
    ("ropek",),
    ("x", "q", 1),
    ("own", "v"),
    ("s3", "q"),
    ("cross", "v"),
    ("a", "v", 1),
    ("b", "v", 1),
    ("x", "q", 2),
    ("s4", "q"),
    ("c", "v", 1),
    ("a", "v", 2),
    ("x", "q", 3),
    ("pq", 1),
    ("b", "v", 2),
    ("c", "v", 2),
    ("pq", 2),
    ("x", "v", 1),
    ("own", "o"),
    ("last", "q"),
    ("pq", 3),
    ("s3", "v"),
    ("pq", 4),
    ("ropeq",),
    ("x", "v", 2),
)
BETWEEN = (
    (),
    (("cross", "o"), ("a", "o", 1), ),
    (("s4", "v"), ("x", "v", 3), ("b", "o", 1), ("c", "o", 1), ),
    (),
    (("last", "v"), ),
    (("a", "o", 2), ("b", "o", 2), ),
    (("c", "o", 2), ("x", "o", 1), ),
)
AFTER = (
    ("fin",),
    ("comp", 1),
    ("comp", 3),
    ("comp", 0),
    ("comp", 2),
    ("s3", "o"),
    ("x", "o", 2),
    ("pair", 3),
    ("pair", 0),
    ("s4", "o"),
    ("comp", 5),
    ("pair", 2),
    ("x", "o", 3),
    ("comp", 4),
    ("across", 3),
    ("pair", 5),
    ("pair", 1),
    ("comp", 6),
    ("last", "o"),
    ("comp", 7),
    ("pair", 4),
    ("done", 3),
    ("across", 5),
    ("pair", 7),
    ("across", 0),
    ("pair", 6),
    ("across", 2),
    ("across", 4),
    ("across", 1),
    ("across", 7),
    ("across", 6),
    ("done", 5),
    ("done", 4),
    ("done", 0),
    ("done", 2),
    ("done", 1),
    ("done", 6),
    ("done", 7),
)
SCALE2 = HEAD_DIM**-0.5 * 1.4426950408889634


def wrap(value, size):
    return lax.rem(value + size, size)


class Gather:
    def __init__(self, kind, buf, rows, place, recv, sib_sem, send_sem):
        self.kind, self.buf, self.rows, self.half = kind, buf, rows, rows // 2
        self.x, self.z, self.c, self.head = place
        self.recv, self.sib_sem, self.send_sem = recv, sib_sem, send_sem
        self.zp = self.at(self.x, 1)
        self.zm = self.at(self.x, -1)
        self.xp = self.at(1 - self.x, 0)
        self.sib = (self.x * ZS + self.z) * 2 + 1 - self.c

    def at(self, x, dz):
        return (x * ZS + wrap(self.z + dz, ZS)) * 2 + self.c

    def copy(self, s, part, dev, sem):
        ref = self.buf.at[pl.ds(pl.multiple_of(s * self.rows + part * self.half, 16), self.half)]
        return pltpu.make_async_remote_copy(
            src_ref=ref,
            dst_ref=ref,
            send_sem=self.send_sem.at[self.kind],
            recv_sem=sem,
            device_id=(dev, self.head),
            device_id_type=MESH,
        )

    def sem(self, s, part):
        return self.recv.at[self.kind, lax.div(s, 2), part]

    def send(self, k, other, s, part, *devs):
        for dev in devs:
            self.copy(s, part, dev, self.sem(s, part)).start()
        self.copy(s, part, self.sib, self.sib_sem.at[self.kind, k + 5 * other]).start()

    def relay(self, k, other, dz, part, *devs):
        s = self.at(1 - self.x if other else self.x, dz)
        self.copy(s, part, self.sib, self.sem(s, part)).wait_recv()
        self.send(k, other, s, part, *devs)

    def own(self):
        for part in (0, 1):
            self.send(0, 0, self.at(self.x, 0), part, self.zp, self.zm, self.xp)

    def cross(self):
        self.relay(0, 1, 0, 0, self.zp, self.zm)
        self.relay(0, 1, 0, 1)

    def a(self, k):
        self.relay(k, 0, -k, 0, self.zp)
        self.relay(k, 0, k, 0, self.zm)

    def b(self, k):
        self.relay(k, 0, -k, 1, self.zp, self.xp)
        self.relay(k, 0, k, 1, self.zm, self.xp)

    def c2(self, k):
        self.relay(k, 1, -k, 0, self.zp)
        self.relay(k, 1, k, 0, self.zm)

    def x2(self, k):
        self.relay(k, 1, -k, 1)
        self.relay(k, 1, k, 1)

    def s3(self):
        self.relay(3, 0, -3, 0, self.zp)
        self.relay(3, 0, 3, 1, self.zm, self.xp)
        self.relay(3, 0, -3, 1, self.xp)
        self.relay(3, 0, 3, 0)
        self.relay(3, 1, -3, 0)
        self.relay(3, 1, 3, 0)

    def s4(self):
        self.relay(4, 0, 4, 0, self.xp)
        self.relay(4, 0, 4, 1, self.xp)

    def last(self):
        self.relay(4, 1, 4, 0)
        self.relay(4, 1, 4, 1)

    def sibling(self, k, *others):
        for other in others:
            part = self.buf.at[pl.ds(0, (1 if k in (0, 4) else 2) * self.rows)]
            pltpu.make_async_copy(part, part, self.sib_sem.at[self.kind, k + 5 * other]).wait()

    def drain(self):
        part = self.buf.at[pl.ds(0, 31 * self.rows)]
        pltpu.make_async_copy(part, part, self.send_sem.at[self.kind]).wait()


def rotated(values, cs, sn):
    return values * cs + pltpu.roll(values, HEAD_DIM // 2, 1) * sn


def kernel(
    hidden, gain_hbm, bq_hbm, bk_hbm, bv_hbm, wq_in, wk_in, wv_in, wo_in, table_hbm, out_hbm,
    hid, wkv, wq, kv, wo, kacc, qacc, qs, cs, sn, tmp, att32, att, terms, r1, r2, xs, xr, tot, keep,
    scores0, scores1, high, acc, vecs, out, out_sem, att_rows, gain_in, bq_in, bk_in, bv_in, table, x_terms, x_recv, x_sum, x_wide, x_r1, x_r2, local, recv, sib_sem, send_sem, rsem, r_send,
):
    s = lax.axis_index("seq")
    head = lax.axis_index("head")
    c = lax.rem(s, 2)
    chip = lax.div(s, 2)
    z = lax.rem(chip, ZS)
    x = lax.div(chip, ZS)
    y = lax.rem(head, YS)
    xh = lax.div(head, YS)
    place = (x, z, c, head)
    gather = functools.partial(Gather, place=place, recv=recv, sib_sem=sib_sem, send_sem=send_sem)
    g_kv_w = gather(0, wkv, 256)
    g_q_w = gather(1, wq, 256)
    g_kv = gather(2, kv, ROWS)
    g_o_w = gather(3, wo, 512)
    yp = xh * YS + wrap(y + 1, YS)
    ym = xh * YS + wrap(y - 1, YS)
    xhp = (1 - xh) * YS + y

    mine = pl.ds(pl.multiple_of(s * 256, 256), 256)
    mine_o = pl.ds(pl.multiple_of(s * 512, 512), 512)
    copies = [
        pltpu.make_async_copy(wk_in, wkv.at[mine, pl.ds(0, 128)], local.at[0]),
        pltpu.make_async_copy(wv_in, wkv.at[mine, pl.ds(128, 128)], local.at[1]),
        pltpu.make_async_copy(wq_in, wq.at[mine], local.at[2]),
        pltpu.make_async_copy(hidden, hid, local.at[3]),
        pltpu.make_async_copy(wo_in, wo.at[mine_o], local.at[4]),
        pltpu.make_async_copy(gain_hbm, gain_in, local.at[5]),
        pltpu.make_async_copy(bq_hbm, bq_in, local.at[6]),
        pltpu.make_async_copy(bk_hbm, bk_in, local.at[7]),
        pltpu.make_async_copy(bv_hbm, bv_in, local.at[8]),
        pltpu.make_async_copy(table_hbm, table, local.at[9]),
    ]
    barrier = pltpu.get_barrier_semaphore()
    for dev in (g_q_w.zp, g_q_w.zm, g_q_w.xp, g_q_w.sib):
        pl.semaphore_signal(barrier, inc=1, device_id=(dev, head), device_id_type=MESH)
    for dev in (yp, ym, xhp):
        pl.semaphore_signal(barrier, inc=1, device_id=(s, dev), device_id_type=MESH)
    for copy in copies:
        copy.start()
    copies[0].wait()
    copies[1].wait()
    copies[2].wait()
    pl.semaphore_wait(barrier, 7)
    kinds = {"k": g_kv_w, "q": g_q_w, "v": g_kv, "o": g_o_w}

    def norm(chunk):
        if chunk == 0:
            tables()
            copies[3].wait()

        @pl.loop(3 * chunk, 3 * chunk + 3)
        def _(i):
            rows = pl.ds(pl.multiple_of(i * 16, 16), 16)
            squares = jnp.zeros((16, 1024), F32)
            for j in range(8):
                part = hid[rows, pl.ds(j * 1024, 1024)].astype(F32)
                squares = squares + part * part
            inverse = lax.rsqrt(jnp.sum(squares, axis=-1, keepdims=True) * (1.0 / D) + EPSILON)
            for j in range(8):
                cols = pl.ds(j * 1024, 1024)
                part = hid[rows, cols].astype(F32)
                hid[rows, cols] = (part * inverse * vecs[:, cols]).astype(BF16)

    def tables():
        for copy in copies[5:]:
            copy.wait()
        for i in range(D // HEAD_DIM):
            vecs[:, pl.ds(i * HEAD_DIM, HEAD_DIM)] = gain_in[pl.ds(i, 1), :].astype(F32)
        for i in range(4):
            vecs[:, pl.ds(D + i * HEAD_DIM, HEAD_DIM)] = bq_in[pl.ds(i, 1), :].astype(F32)
        vecs[:, pl.ds(D + 512, HEAD_DIM)] = bk_in[...].astype(F32)
        vecs[:, pl.ds(D + 640, HEAD_DIM)] = bv_in[...].astype(F32)
        cos_row, sin_row = table[0:ROWS, :], table[ROWS : 2 * ROWS, :]
        cos_first = table[pl.ds(2 * ROWS + s, 1), :]
        sin_first = table[pl.ds(2 * ROWS + SEQ + s, 1), :]
        cs[...] = cos_first * cos_row - sin_first * sin_row
        sine = sin_first * cos_row + cos_first * sin_row
        lane = lax.broadcasted_iota(jnp.int32, (ROWS, HEAD_DIM), 1)
        sn[...] = jnp.where(lane < HEAD_DIM // 2, -sine, sine)

    def project(gather, sums, k):
        gather.sibling(k, 0, 1)
        total = None
        for other in (0, 1):
            for dz in (0,) if k == 0 else (4,) if k == 4 else (-k, k):
                place = lax.div(gather.at(1 - x if other else x, dz), 2)
                depth = pl.ds(pl.multiple_of(place * 512, 512), 512)
                term = jnp.dot(hid[:, depth], gather.buf[depth, :], preferred_element_type=F32)
                total = term if total is None else total + term
        sums[...] = total if k == 0 else sums[...] + total

    def store_kv():
        own_kv = pl.ds(pl.multiple_of(s * ROWS, 16), ROWS)
        bk = vecs[:, D + 512 : D + 640]
        bv = vecs[:, D + 640 : D + 768]
        kv[own_kv, 0:128] = rotated(kacc[:, 0:128] + bk, cs[...], sn[...]).astype(BF16)
        kv[own_kv, 128:256] = (kacc[:, 128:256] + bv).astype(BF16)

    def store_q():
        for j in range(4):
            cols = pl.ds(j * HEAD_DIM, HEAD_DIM)
            value = qacc[:, cols] + vecs[:, pl.ds(D + j * HEAD_DIM, HEAD_DIM)]
            qs[pl.ds(j * ROWS, ROWS), :] = rotated(value, cs[...], sn[...]).astype(BF16)

    last_block = lax.div(s, 4)
    score_bufs = (scores0, scores1)

    def set_scores(j, block):
        keys = kv[pl.ds(pl.multiple_of(block * KBLOCK, KBLOCK), KBLOCK), 0:128]
        score_bufs[j % 2][...] = lax.dot_general(
            qs[pl.ds(j * ROWS, ROWS), :], keys, (((1,), (1,)), ((), ())), preferred_element_type=F32
        )

    def attend(block, following, diagonal):
        values = kv[pl.ds(pl.multiple_of(block * KBLOCK, KBLOCK), KBLOCK), 128:256]
        for j in range(4):
            rows = pl.ds(j * ROWS, ROWS)
            set_scores((j + 1) % 4, block if j < 3 else following)
            scores = score_bufs[j % 2][...]
            if diagonal:
                query_pos = s * ROWS + lax.broadcasted_iota(jnp.int32, (ROWS, KBLOCK), 0)
                key_pos = block * KBLOCK + lax.broadcasted_iota(jnp.int32, (ROWS, KBLOCK), 1)
                scores = jnp.where(query_pos >= key_pos, scores, -jnp.inf)
            new_high = jnp.broadcast_to(jnp.max(scores, axis=-1, keepdims=True), (ROWS, HEAD_DIM))
            if not diagonal:
                old_high = high[rows, :]
                new_high = jnp.maximum(old_high, new_high)
            probs = jnp.exp2((scores - jnp.tile(new_high, (1, KBLOCK // HEAD_DIM))) * SCALE2)
            part = probs[:, 0:HEAD_DIM]
            for n in range(1, KBLOCK // HEAD_DIM):
                part = part + probs[:, n * HEAD_DIM : (n + 1) * HEAD_DIM]
            mixed = jnp.dot(probs.astype(BF16), values, preferred_element_type=F32)
            if not diagonal:
                fade = jnp.exp2((old_high - new_high) * SCALE2)
                mixed = acc[rows, 0:HEAD_DIM] * fade + mixed
                part = acc[rows, HEAD_DIM : 2 * HEAD_DIM] * fade + part
            acc[rows, 0:HEAD_DIM] = mixed
            acc[rows, HEAD_DIM : 2 * HEAD_DIM] = part
            high[rows, :] = new_high

    def block_at(i):
        own = (i < 3) | (i == 6)
        column = jnp.where(own, x, 1 - x)
        step = jnp.where(i >= 6, 2, jnp.where(i < 3, jnp.where(i == 2, 1, -i), jnp.where(i == 5, 1, 3 - i)))
        return 4 * column + lax.rem(lax.div(z, 2) + step + 4, 4)

    def arrived(i):
        for k, other in {0: ((0, 0), (1, 0), (2, 0), (3, 0)), 2: ((0, 1), (1, 1)), 3: ((2, 1), (3, 1)), 5: ((4, 0),), 6: ((4, 1),)}.get(i, ()):
            g_kv.sibling(k, other)

    def finish_attention():
        att32[...] = jnp.zeros(att32.shape, F32)
        for j in range(4):
            rows = pl.ds(j * ROWS, ROWS)
            tmp[...] = acc[rows, 0:HEAD_DIM] / jnp.sum(
                acc[rows, HEAD_DIM : 2 * HEAD_DIM], axis=-1, keepdims=True
            )
            att_rows[:, pl.ds(j * HEAD_DIM, HEAD_DIM)] = tmp[...].astype(BF16)
            for h in range(8):
                spot = PADROWS * (h % YS) + OWN * (h // YS)
                att32[pl.ds(spot, OWN), pl.ds(j * HEAD_DIM, HEAD_DIM)] = tmp[pl.ds(h * OWN, OWN), :]
        att[...] = att32[...].astype(BF16)

    y2 = wrap(y + 2, YS)
    y_next = wrap(y + 1, YS)
    y_prev = wrap(y - 1, YS)

    def move(src, dst, kind, g, dev):
        return pltpu.make_async_remote_copy(
            src_ref=src,
            dst_ref=dst,
            send_sem=r_send.at[kind, g],
            recv_sem=rsem.at[kind, g],
            device_id=(s, dev),
            device_id_type=MESH,
        )

    def first(g, kind):
        half = COLS[g] // 2
        cols = pl.ds(BASE[g] + kind * half, half)
        near = r1.at[kind, :, pl.ds(BASE[g] // 2, half)]
        return move(terms.at[y2, :, cols], near, kind, g, ym if kind else yp)

    def second(g, kind):
        cols = pl.ds(BASE[g], COLS[g])
        row = y_prev if kind else y_next
        return move(terms.at[row, :, cols], r2.at[kind, :, cols], 2 + kind, g, ym if kind else yp)

    def third(g):
        cols = pl.ds(BASE[g], COLS[g])
        return move(xs.at[:, cols], xr.at[:, cols], 4, g, xhp)

    def slot_of(g, i):
        k = DISTANCE[g]
        ends = k in (0, 4)
        other = lax.div(i, 2) if ends else 1 - g % 2
        side = 0 if ends else lax.div(i, 2)
        core = lax.rem(i, 2)
        xx = x + other - 2 * x * other
        return (xx * ZS + wrap(z + k - 2 * k * side, ZS)) * 2 + c + core - 2 * c * core

    def shards_in(g):
        k = DISTANCE[g]
        g_o_w.sibling(k, *((0, 1) if k in (0, 4) else (1 - g % 2,)))

    def compute(g):
        shards_in(g)

        @pl.loop(0, COLS[g] // 256)
        def _(i):
            depth = pl.ds(pl.multiple_of(slot_of(g, i) * 512, 512), 512)
            cols = pl.ds(pl.multiple_of(BASE[g] + i * 256, 256), 256)
            term = jnp.dot(att[...], wo[depth, :], preferred_element_type=F32).astype(BF16)
            for k in range(YS):
                terms[k, :, cols] = term[PADROWS * k : PADROWS * k + 2 * OWN]

        first(g, 0).start()
        first(g, 1).start()

    def pair(g):
        for kind in (0, 1):
            first(g, kind).wait_recv()
            row = y_prev if kind else y_next
            half = COLS[g] // 2
            cols = pl.ds(BASE[g] + kind * half, half)
            near = r1[kind, :, pl.ds(BASE[g] // 2, half)].astype(F32)
            terms[row, :, cols] = (terms[row, :, cols].astype(F32) + near).astype(BF16)
            second(g, kind).start()

    def across(g):
        second(g, 0).wait_recv()
        second(g, 1).wait_recv()
        cols = pl.ds(BASE[g], COLS[g])
        part = tot.at[:, pl.ds(0, COLS[g])]
        part[...] = terms[y, :, cols].astype(F32) + r2[0, :, cols].astype(F32) + r2[1, :, cols].astype(F32)
        low, high_rows = part[0:OWN, :], part[OWN : 2 * OWN, :]
        lower = xh == 0
        xs[:, cols] = jnp.where(lower, high_rows, low).astype(BF16)
        keep[:, cols] = jnp.where(lower, low, high_rows)
        third(g).start()

    def done(g):
        third(g).wait_recv()

        @pl.loop(0, COLS[g] // 256)
        def _(i):
            cols = pl.ds(pl.multiple_of(BASE[g] + i * 256, 256), 256)
            there = pl.ds(pl.multiple_of(slot_of(g, i) * 256, 256), 256)
            out[:, there] = (keep[:, cols] + xr[:, cols].astype(F32)).astype(BF16)
            pltpu.make_async_copy(out.at[:, there], out_hbm.at[:, there], out_sem).start()

    def x_cols(g):
        return pl.ds(XBASE[g], COLS[g])

    def x_first(g):
        return move(x_terms.at[1 - xh, :, x_cols(g)], x_recv.at[:, x_cols(g)], 4, g, xhp)

    def x_second(g, kind):
        half = COLS[g] // 2
        near = x_r1.at[kind, :, pl.ds(XBASE[g] // 2, half)]
        return move(x_sum.at[y2, :, pl.ds(XBASE[g] + kind * half, half)], near, kind, g, ym if kind else yp)

    def x_third(g, kind):
        row = y_prev if kind else y_next
        return move(x_sum.at[row, :, x_cols(g)], x_r2.at[kind, :, x_cols(g)], 2 + kind, g, ym if kind else yp)

    def x_compute(g):
        shards_in(g)

        @pl.loop(0, COLS[g] // 256)
        def _(i):
            depth = pl.ds(pl.multiple_of(slot_of(g, i) * 512, 512), 512)
            cols = pl.ds(pl.multiple_of(XBASE[g] + i * 256, 256), 256)
            term = jnp.dot(att_rows[...], wo[depth, :], preferred_element_type=F32).astype(BF16)
            for k in range(2):
                x_terms[k, :, cols] = term[ROWS // 2 * k : ROWS // 2 * (k + 1)]

        x_first(g).start()

    def x_pair(g):
        x_first(g).wait_recv()
        wide = x_wide.at[:, pl.ds(0, COLS[g])]
        wide[...] = x_terms[xh, :, x_cols(g)].astype(F32) + x_recv[:, x_cols(g)].astype(F32)
        for k in range(YS):
            x_sum[k, :, x_cols(g)] = wide[pl.ds(OWN * k, OWN), :].astype(BF16)
        x_second(g, 0).start()
        x_second(g, 1).start()

    def x_across(g):
        half = COLS[g] // 2
        for kind in (0, 1):
            x_second(g, kind).wait_recv()
            row = y_prev if kind else y_next
            cols = pl.ds(XBASE[g] + kind * half, half)
            near = x_r1[kind, :, pl.ds(XBASE[g] // 2, half)].astype(F32)
            x_sum[row, :, cols] = (x_sum[row, :, cols].astype(F32) + near).astype(BF16)
            x_third(g, kind).start()

    def x_done(g):
        x_third(g, 0).wait_recv()
        x_third(g, 1).wait_recv()

        @pl.loop(0, COLS[g] // 256)
        def _(i):
            cols = pl.ds(pl.multiple_of(XBASE[g] + i * 256, 256), 256)
            there = pl.ds(pl.multiple_of(slot_of(g, i) * 256, 256), 256)
            value = x_sum[y, :, cols].astype(F32) + x_r2[0, :, cols].astype(F32)
            out[:, there] = (value + x_r2[1, :, cols].astype(F32)).astype(BF16)
            pltpu.make_async_copy(out.at[:, there], out_hbm.at[:, there], out_sem).start()

    x_stages = {"comp": x_compute, "pair": x_pair, "across": x_across, "done": x_done}

    def run(op):
        name, rest = op[0], op[1:]
        if name in ("own", "cross", "s3", "s4", "last"):
            if op == ("own", "o"):
                copies[4].wait()
            getattr(kinds[rest[0]], name)()
        elif name in ("a", "b"):
            getattr(kinds[rest[0]], name)(rest[1])
        elif name in ("c", "x"):
            getattr(kinds[rest[0]], name + "2")(rest[1])
        elif name == "pk":
            project(g_kv_w, kacc, rest[0])
        elif name == "pq":
            project(g_q_w, qacc, rest[0])
        elif name in x_stages and rest[0] in XBASE:
            x_stages[name](rest[0])
        else:
            simple[name](*rest)

    simple = {
        "norm": norm,
        "ropek": store_kv,
        "ropeq": store_q,
        "fin": finish_attention,
        "comp": compute,
        "pair": pair,
        "across": across,
        "done": done,
    }
    for op in BEFORE:
        run(op)
    arrived(0)
    set_scores(0, last_block)
    attend(last_block, block_at(1), True)

    @pl.loop(1, 8)
    def _(i):
        for n, ops in enumerate(BETWEEN):

            @pl.when(i == n + 1)
            def _():
                for op in ops:
                    run(op)
                arrived(n + 1)

        block, following = block_at(i), block_at(jnp.minimum(i + 1, 7))

        @pl.when(block < last_block)
        def _():
            attend(block, following, False)

        @pl.when(block >= last_block)
        def _():
            set_scores(0, following)

    for op in AFTER:
        run(op)

    for g in range(GROUPS):
        one, two, three = (x_second, x_third, x_first) if g in XBASE else (first, second, third)
        for kind in (0, 1):
            one(g, kind).wait_send()
            two(g, kind).wait_send()
        three(g).wait_send()
    for g in (g_kv_w, g_q_w, g_kv, g_o_w):
        g.drain()
    pltpu.make_async_copy(out, out_hbm, out_sem).wait()


def rotary_table():
    half_dim = HEAD_DIM // 2
    freq = ROPE_BASE ** (-2.0 * np.arange(half_dim) / HEAD_DIM)
    rows = np.arange(ROWS)[:, None] * freq
    firsts = ROWS * np.arange(SEQ)[:, None] * freq
    parts = (np.cos(rows), np.sin(rows), np.cos(firsts), np.sin(firsts))
    return np.tile(np.concatenate(parts, axis=0), (1, 2)).astype(np.float32)


def local(hidden, norm_gain, w_query, w_key, w_value, bias_query, bias_key, bias_value, w_out):
    vmem = pl.BlockSpec(memory_space=pltpu.VMEM)
    hbm = pl.BlockSpec(memory_space=pl.ANY)
    dma = pltpu.SemaphoreType.DMA
    return pl.pallas_call(
        kernel,
        name="layer",
        out_shape=jax.ShapeDtypeStruct((OWN, D), BF16),
        in_specs=[hbm] * 10,
        out_specs=hbm,
        scratch_shapes=[
            pltpu.VMEM((ROWS, D), BF16),
            pltpu.VMEM((D, 256), BF16),
            pltpu.VMEM((D, 512), BF16),
            pltpu.VMEM((SEQ * ROWS, 256), BF16),
            pltpu.VMEM((SEQ * 512, 256), BF16),
            pltpu.VMEM((ROWS, 256), F32),
            pltpu.VMEM((ROWS, 512), F32),
            pltpu.VMEM((4 * ROWS, HEAD_DIM), BF16),
            pltpu.VMEM((ROWS, HEAD_DIM), F32),
            pltpu.VMEM((ROWS, HEAD_DIM), F32),
            pltpu.VMEM((ROWS, HEAD_DIM), F32),
            pltpu.VMEM((YS * PADROWS, 512), F32),
            pltpu.VMEM((YS * PADROWS, 512), BF16),
            pltpu.VMEM((YS, 2 * OWN, D), BF16),
            pltpu.VMEM((2, 2 * OWN, D // 2), BF16),
            pltpu.VMEM((2, 2 * OWN, D), BF16),
            pltpu.VMEM((OWN, D), BF16),
            pltpu.VMEM((OWN, D), BF16),
            pltpu.VMEM((2 * OWN, 1024), F32),
            pltpu.VMEM((OWN, D), F32),
            pltpu.VMEM((ROWS, KBLOCK), F32),
            pltpu.VMEM((ROWS, KBLOCK), F32),
            pltpu.VMEM((4 * ROWS, HEAD_DIM), F32),
            pltpu.VMEM((4 * ROWS, 2 * HEAD_DIM), F32),
            pltpu.VMEM((1, D + 768), F32),
            pltpu.VMEM((OWN, D), BF16),
            dma,
            pltpu.VMEM((ROWS, 512), BF16),
            pltpu.VMEM((D // HEAD_DIM, HEAD_DIM), BF16),
            pltpu.VMEM((4, HEAD_DIM), BF16),
            pltpu.VMEM((1, HEAD_DIM), BF16),
            pltpu.VMEM((1, HEAD_DIM), BF16),
            pltpu.VMEM((2 * ROWS + 2 * SEQ, HEAD_DIM), F32),
            pltpu.VMEM((2, ROWS // 2, XCOLS), BF16),
            pltpu.VMEM((ROWS // 2, XCOLS), BF16),
            pltpu.VMEM((YS, OWN, XCOLS), BF16),
            pltpu.VMEM((ROWS // 2, 1024), F32),
            pltpu.VMEM((2, OWN, XCOLS // 2), BF16),
            pltpu.VMEM((2, OWN, XCOLS), BF16),
            dma((10,)),
            dma((4, 16, 2)),
            dma((4,10)),
            dma((4,)),
            dma((5, GROUPS)),
            dma((5, GROUPS)),
        ],
        compiler_params=pltpu.CompilerParams(
            collective_id=0, has_side_effects=True, vmem_limit_bytes=66 * 1000 * 1000
        ),
    )(
        hidden, norm_gain.reshape(-1, HEAD_DIM), bias_query.reshape(-1, HEAD_DIM),
        bias_key.reshape(-1, HEAD_DIM), bias_value.reshape(-1, HEAD_DIM),
        w_query, w_key, w_value, w_out, jnp.asarray(rotary_table()),
    )


def solution(mesh):
    in_specs = (
        P("seq", None),
        P(),
        P("seq", "head"),
        P("seq", "head"),
        P("seq", "head"),
        P("head"),
        P("head"),
        P("head"),
        P("head", "seq"),
    )
    out_specs = P(("seq", "head"), None)
    return jax.shard_map(local, mesh=mesh, in_specs=in_specs, out_specs=out_specs, check_vma=False)
```
